256 devices in a mesh: row: 8 (over y, z_lo), col: 4 (over x), band: 8 (over z_hi, core).
Axes of the slice: x: 4, y: 4, z: 8 (z_hi: 4, z_lo: 2; z = z_hi * 2 + z_lo), core: 2. Of those that a mesh axis runs over, the one named last changes fastest.
Arguments:
- noisy: float32 [224, 128, 4096], P('band', 'row', 'col'), may hold values from -4 to 4
- weight_map: float32 [128, 4096], P('row', 'col'), may hold values from 1.5 to 12
Outputs:
- denoised: float32 [224, 128, 4096], P('band', 'row', 'col')
The draws below stay inside these ranges and needn't reach their ends.
All inputs are finite; a program needn't handle non-finite values.
Results may differ from the reference program's by a relative error of at most 0.0001.
Values sent between devices are 32-bit elements; how exact they have to be, the bound alone decides.
No kernel may reach another device: no remote copies, remote signals or barrier semaphores. Data moves between devices by JAX's collectives and lax.ppermute only.
A program may use at most 64 MiB of HBM per device.

```python
import math
import jax
import jax.numpy as jnp
from jax import lax

BANDS = 224
COLS = 4096
ITERS = 4
ROWS = 128


def draw_noisy(key, part):
    key_center, key_texture = jax.random.split(jax.random.fold_in(key, 17))
    center = jax.random.randint(key_center, (), 0, BANDS).astype(jnp.float32)
    spread = BANDS / 16.0
    texture = jnp.clip(jax.random.normal(key_texture, (BANDS, ROWS, COLS), jnp.float32), -4.0, 4.0)
    offset = (jnp.arange(BANDS, dtype=jnp.float32) - center) / spread
    profile = 0.1 + 0.9 * jnp.exp(-0.5 * offset * offset)
    return (profile[:, None, None] * texture).astype(jnp.float32)


def shard_levels(key, extent, cuts, low, top_value):
    level = 1.0
    for dim, shards_of in cuts:
        steps = jax.random.uniform(jax.random.fold_in(jax.random.fold_in(key, 6), dim), (shards_of,), jnp.float32, low / len(cuts), top_value / len(cuts))
        level = level * jnp.repeat(jnp.exp(steps), extent[dim] // shards_of).reshape((-1,) + (1,) * (len(extent) - 1 - dim))
    return level


def setup_inputs(seed: int = 0) -> dict:
    key_of = jax.random.split(jax.random.key(seed), 3)
    noisy = draw_noisy(jax.random.fold_in(key_of[2], 71), 0)
    weight_map = jnp.clip(jnp.exp(math.log(12.0) - 2.0794415 * jax.random.uniform(key_of[1], (ROWS, COLS), jnp.float32) ** shard_levels(key_of[1], (ROWS, COLS), ((0, 8), (1, 4)), -0.2, 0.2)), 1.5, 12.0)
    return {"noisy": noisy, "weight_map": weight_map}


dual_step = 0.35
primal_step = 0.35

def forward_diff(field):
    zeros_row = jnp.zeros_like(field[:, :1, :])
    zeros_col = jnp.zeros_like(field[:, :, :1])
    grad_x = jnp.concatenate([field[:, 1:, :] - field[:, :-1, :], zeros_row], axis=1)
    grad_y = jnp.concatenate([field[:, :, 1:] - field[:, :, :-1], zeros_col], axis=2)
    return (grad_x, grad_y)

def divergence(first, second):
    masked_a = first.at[:, -1, :].set(0.0)
    masked_b = second.at[:, :, -1].set(0.0)
    above = jnp.concatenate([jnp.zeros_like(masked_a[:, :1, :]), masked_a[:, :-1, :]], axis=1)
    left = jnp.concatenate([jnp.zeros_like(masked_b[:, :, :1]), masked_b[:, :, :-1]], axis=2)
    return masked_a - above + (masked_b - left)

def reference(noisy, weight_map):
    groups = math.gcd(BANDS, 8)
    rows = noisy.shape[1]
    cols = noisy.shape[2]
    source = noisy.reshape(groups, BANDS // groups, rows, cols)
    primal = source
    extra = source
    dual_x = jnp.zeros_like(source)
    dual_y = jnp.zeros_like(source)
    for step in range(ITERS):

        def dual_part(items):
            ubar, first, second = items
            grad_x, grad_y = forward_diff(ubar)
            qx = first + dual_step * grad_x
            qy = second + dual_step * grad_y
            return (qx, qy, lax.optimization_barrier(jnp.sum(qx * qx + qy * qy, axis=0)))
        qxs, qys, partial_value = lax.map(dual_part, (extra, dual_x, dual_y))
        squares = lax.optimization_barrier(jnp.sum(partial_value, axis=0))
        scale = weight_map / jnp.maximum(weight_map, jnp.sqrt(1.0 + squares))

        def primal_part(items):
            qx, qy, older, given = items
            first = scale * qx
            second = scale * qy
            newer = (older + primal_step * divergence(first, second) + primal_step * given) / (1.0 + primal_step)
            return (first, second, newer, 2.0 * newer - older)
        dual_x, dual_y, primal, extra = lax.map(primal_part, (qxs, qys, primal, source))
    return primal.reshape(BANDS, rows, cols)
```

```python
import jax
import jax.numpy as jnp
from jax import lax
from jax.experimental import pallas as pl
from jax.experimental.pallas import tpu as pltpu
from jax.sharding import PartitionSpec as P

ITERS = 4
M = ITERS
LANES = 128
SIGMA = 0.35
TAU = 0.35


F32 = jnp.float32
VM = pl.BlockSpec(memory_space=pltpu.VMEM)
SM = pl.BlockSpec(memory_space=pltpu.SMEM)
PARAMS = pltpu.CompilerParams(vmem_limit_bytes=16 * 1024 * 1024)


def call(body, outs, ins, n_smem=0, aliases=None, scratch=(), flops=0):
    return pl.pallas_call(
        body,
        out_shape=[pltpu.VMEM(s, F32) for s in outs],
        in_specs=[SM] * n_smem + [VM] * (len(ins) - n_smem),
        out_specs=[VM] * len(outs),
        scratch_shapes=list(scratch),
        input_output_aliases=aliases or {},
        compiler_params=PARAMS,
        cost_estimate=pl.CostEstimate(flops=flops, bytes_accessed=0, transcendentals=0),
    )(*ins)


def lane_iota(shape):
    return lax.broadcasted_iota(jnp.int32, shape, len(shape) - 1)


class Sizes:
    def __init__(self, bands, rows, cols):
        self.b = bands
        self.nb = 2 * bands
        self.bt = self.nb // 8
        self.r = rows
        self.c = cols // 2
        self.er = rows + 2 * M
        self.ec = self.c + LANES
        self.full = self.b // 8 * 8
        self.rest = self.b - self.full


def pack_lanes(tiles, first, width):
    per = LANES // width
    lane = lane_iota((8, LANES))
    out = []
    for v in range(0, len(tiles), per):
        acc = None
        for p, tile in enumerate(tiles[v : v + per]):
            moved = pltpu.roll(tile, (p * width - first) % LANES, axis=1)
            acc = moved if acc is None else jnp.where(lane // width == p, moved, acc)
        out.append(acc)
    return out


def assemble(z, core, keep, recv, w, ne, col_l, col_r, row_u, row_d):
    f, q = z.full, z.rest

    def join(first, second):
        def put(r, _):
            e = r + M
            ne[e, 0:f, 0 : z.c] = first[r, 0:f, :]
            ne[e, f : 2 * f, 0 : z.c] = second[r, 0:f, :]
            ne[e, 2 * f : 2 * f + q, 0 : z.c] = first[r, f : z.b, :]
            ne[e, 2 * f + q : z.nb, 0 : z.c] = second[r, f : z.b, :]
            return 0

        lax.fori_loop(0, z.r, put, 0)

    pl.when(core[0] == 0)(lambda: join(keep, recv))
    pl.when(core[0] == 1)(lambda: join(recv, keep))
    left = [ne[M + r, 8 * t : 8 * t + 8, 0:LANES] for r in range(z.r) for t in range(z.bt)]
    left += [w[8 * t : 8 * t + 8, 0:LANES] for t in range(z.r // 8)]
    right = [ne[M + r, 8 * t : 8 * t + 8, z.c - LANES : z.c] for r in range(z.r) for t in range(z.bt)]
    right += [w[8 * t : 8 * t + 8, z.c - LANES : z.c] for t in range(z.r // 8)]
    for v, tile in enumerate(pack_lanes(left, 0, M)):
        col_l[v] = tile
    for v, tile in enumerate(pack_lanes(right, LANES - M, M)):
        col_r[v] = tile
    for r in range(M):
        for t in range(z.bt):
            row_u[r * z.bt + t] = ne[M + r, 8 * t : 8 * t + 8, 0 : z.c]
            row_d[r * z.bt + t] = ne[z.r + r, 8 * t : 8 * t + 8, 0 : z.c]
    row_u[M * z.bt] = w[0:8, :]
    row_d[M * z.bt] = w[z.r - 8 : z.r, :]


def frame_cols(z, ne_in, w, from_r, from_l, ne, wx, cor_u, cor_d):
    lane = lane_iota((8, LANES))
    per = LANES // M
    units = z.r * z.bt + z.r // 8
    tiles = []
    for k in range(units):
        v, p = divmod(k, per)
        hi = pltpu.roll(from_r[v], (-p * M) % LANES, axis=1)
        lo = pltpu.roll(from_l[v], (LANES - M - p * M) % LANES, axis=1)
        tiles.append(jnp.where(lane < M, hi, jnp.where(lane >= LANES - M, lo, 0.0)))
    for r in range(z.r):
        for t in range(z.bt):
            ne[M + r, 8 * t : 8 * t + 8, z.c : z.ec] = tiles[r * z.bt + t]
    wx[0:M, :] = jnp.zeros((M, z.ec), F32)
    wx[M + z.r : z.er, :] = jnp.zeros((M, z.ec), F32)
    wx[M : M + z.r, 0 : z.c] = w[...]
    for t in range(z.r // 8):
        wx[M + 8 * t : M + 8 * t + 8, z.c : z.ec] = tiles[z.r * z.bt + t]
    up = tiles[: M * z.bt] + [tiles[z.r * z.bt]]
    down = tiles[(z.r - M) * z.bt : z.r * z.bt] + [tiles[units - 1]]
    for v, tile in enumerate(pack_lanes(up, LANES - M, 2 * M)):
        cor_u[v] = tile
    for v, tile in enumerate(pack_lanes(down, LANES - M, 2 * M)):
        cor_d[v] = tile


def frame_rows(z, kx, ne_in, wx_in, ky, below, above, cor_b, cor_a, ne, wx, qx, qy, s, acc):
    lane = lane_iota((8, LANES))
    per = LANES // (2 * M)
    units = M * z.bt + 1

    def corner(ref, k):
        v, p = divmod(k, per)
        got = pltpu.roll(ref[v], (LANES - M - p * 2 * M) % LANES, axis=1)
        return jnp.where((lane < M) | (lane >= LANES - M), got, 0.0)

    for r in range(M):
        for t in range(z.bt):
            k = r * z.bt + t
            ne[M + z.r + r, 8 * t : 8 * t + 8, 0 : z.c] = below[k]
            ne[M + z.r + r, 8 * t : 8 * t + 8, z.c : z.ec] = corner(cor_b, k)
            ne[r, 8 * t : 8 * t + 8, 0 : z.c] = above[k]
            ne[r, 8 * t : 8 * t + 8, z.c : z.ec] = corner(cor_a, k)
    wx[...] = wx_in[...]
    wx[M + z.r : z.er, 0 : z.c] = below[units - 1][0:M]
    wx[M + z.r : z.er, z.c : z.ec] = corner(cor_b, units - 1)[0:M]
    wx[0:M, 0 : z.c] = above[units - 1][8 - M : 8]
    wx[0:M, z.c : z.ec] = corner(cor_a, units - 1)[8 - M : 8]
    acc[...] = jnp.zeros_like(acc)
    kyb = jnp.broadcast_to(ky[...], (8, z.ec))

    def band_tile(t, _):
        b = pl.ds(pl.multiple_of(t * 8, 8), 8)
        here = ne[0, b, :]
        for e in range(z.er - 1):
            below_row = ne[e + 1, b, :]
            gx = kx[e] * (below_row - here)
            gy = kyb * (pltpu.roll(here, z.ec - 1, axis=1) - here)
            qx[e, b, :] = gx
            qy[e, b, :] = gy
            acc[e] = acc[e] + (gx * gx + gy * gy)
            here = below_row
        return 0

    lax.fori_loop(0, z.bt, band_tile, 0)
    s[...] = jnp.zeros_like(s)
    for e in range(z.er - 1):
        s[e : e + 1, :] = jnp.sum(acc[e], axis=0, keepdims=True)


def spread_scale(z, lo, hi, wx, s_a, s_b, scl, scale):
    w = wx[...]
    scl[...] = w / jnp.maximum(w, jnp.sqrt(1.0 + (s_a[...] + s_b[...])))
    for e in range(lo, hi):
        scale[e] = jnp.broadcast_to(scl[e : e + 1, :], (8, z.ec))


CARRY = 1.0 / (1.0 + TAU)
GAIN = TAU / (1.0 + TAU)


def step(z, k, kx, ne, wx, ky, u_in, qx_in, qy_in, s_a, s_b, u, qx, qy, s, scl, scale, acc):
    lo, hi = k, z.er - 1 - k
    spread_scale(z, lo, hi, wx, s_a, s_b, scl, scale)
    acc[...] = jnp.zeros_like(acc)
    kyb = jnp.broadcast_to(ky[...], (8, z.ec))

    def band_tile(t, _):
        b = pl.ds(pl.multiple_of(t * 8, 8), 8)
        px0 = scale[lo] * qx_in[lo, b, :]
        py0 = ub0 = None
        for e in range(lo + 1, hi):
            sc = scale[e]
            px = sc * qx_in[e, b, :]
            py = sc * qy_in[e, b, :]
            div = (px - px0) + (py - pltpu.roll(py, 1, axis=1))
            old = u_in[e, b, :]
            if k == 0:
                new = old + GAIN * div
            else:
                new = CARRY * old + GAIN * (div + ne[e, b, :])
            ub = 2.0 * new - old
            u[e, b, :] = new
            if e > lo + 1:
                nx = px0 + kx[e - 1] * (ub - ub0)
                ny = py0 + kyb * (pltpu.roll(ub0, z.ec - 1, axis=1) - ub0)
                qx[e - 1, b, :] = nx
                qy[e - 1, b, :] = ny
                acc[e - 1] = acc[e - 1] + (nx * nx + ny * ny)
            px0, py0, ub0 = px, py, ub
        return 0

    lax.fori_loop(0, z.bt, band_tile, 0)
    s[...] = jnp.zeros_like(s)
    for e in range(lo + 1, hi - 1):
        s[e : e + 1, :] = jnp.sum(acc[e], axis=0, keepdims=True)


def last_step(z, k, core, ne, wx, u_in, qx_in, qy_in, s_a, s_b, keep, send, scl, scale, u):
    lo, hi = k, z.er - 1 - k
    spread_scale(z, lo, hi, wx, s_a, s_b, scl, scale)

    def band_tile(t, _):
        b = pl.ds(pl.multiple_of(t * 8, 8), 8)
        px0 = scale[lo] * qx_in[lo, b, :]
        for e in range(lo + 1, hi):
            sc = scale[e]
            px = sc * qx_in[e, b, :]
            py = sc * qy_in[e, b, :]
            div = (px - px0) + (py - pltpu.roll(py, 1, axis=1))
            new = CARRY * u_in[e, b, :] + GAIN * (div + ne[e, b, :])
            u[e - M, b, :] = new[:, 0 : z.c]
            px0 = px
        return 0

    lax.fori_loop(0, z.bt, band_tile, 0)
    f, q = z.full, z.rest

    def part(first, second):
        def put(r, _):
            first[r, 0:f, :] = u[r, 0:f, :]
            second[r, 0:f, :] = u[r, f : 2 * f, :]
            first[r, f : z.b, :] = u[r, 2 * f : 2 * f + q, :]
            second[r, f : z.b, :] = u[r, 2 * f + q : z.nb, :]
            return 0

        lax.fori_loop(0, z.r, put, 0)

    pl.when(core[0] == 0)(lambda: part(keep, send))
    pl.when(core[0] == 1)(lambda: part(send, keep))


def local(noisy, weight_map):
    z = Sizes(*noisy.shape)
    n_row, n_col, n_band = (lax.axis_size(a) for a in ("row", "col", "band"))
    core = lax.axis_index("band") % 2
    row0 = lax.axis_index("row") * z.r - M
    col0 = lax.axis_index("col") * (2 * z.c) + core * z.c

    grow = row0 + jnp.arange(z.er)
    kx = jnp.where((grow >= 0) & (grow < n_row * z.r - 1), SIGMA, 0.0).astype(F32)
    lane = jnp.arange(z.ec)
    gcol = col0 + jnp.where(lane < z.c + LANES // 2, lane, lane - z.ec)
    ky = jnp.where((gcol >= 0) & (gcol < n_col * 2 * z.c - 1), SIGMA, 0.0).astype(F32)[None]

    swap = [(i, i ^ 1) for i in range(n_band)]
    pair_a = [(i, i ^ 2) for i in range(n_band)]
    chips = n_band // 2
    pair_b = [(i, (((i // 2) - 1 + 2 * ((i // 2) % 2)) % chips) * 2 + i % 2) for i in range(n_band)]
    up = [(i + 1, i) for i in range(n_row - 1)]
    down = [(i, i + 1) for i in range(n_row - 1)]

    def place(col, band):
        return col * n_band + band

    line = [(place(j // 2, 2 * h + j % 2), place((j + 1) // 2, 2 * h + (j + 1) % 2))
            for h in range(chips) for j in range(2 * n_col - 1)]
    to_right = line
    to_left = [(b, a) for a, b in line]

    turned = jnp.swapaxes(noisy, 0, 1)
    keep = lax.dynamic_slice_in_dim(turned, core * z.c, z.c, axis=2)
    send = lax.dynamic_slice_in_dim(turned, (1 - core) * z.c, z.c, axis=2)
    w = lax.dynamic_slice_in_dim(weight_map, core * z.c, z.c, axis=1)
    recv = lax.ppermute(send, "band", swap)

    units = z.r * z.bt + z.r // 8
    n_edge = -(-units // (LANES // M))
    n_corner = -(-(M * z.bt + 1) // (LANES // (2 * M)))
    big = (z.er, z.nb, z.ec)
    flat = (z.er, z.ec)
    edge = (n_edge, 8, LANES)
    bulk = (M * z.bt + 1, 8, z.c)
    corner = (n_corner, 8, LANES)
    cost = z.er * z.nb * z.ec

    ne, col_l, col_r, row_u, row_d = call(
        lambda *a: assemble(z, *a), [big, edge, edge, bulk, bulk], [core[None], keep, recv, w],
        n_smem=1, flops=cost
    )
    below = lax.ppermute(row_u, "row", up)
    above = lax.ppermute(row_d, "row", down)
    from_r = lax.ppermute(col_l, ("col", "band"), to_left)
    from_l = lax.ppermute(col_r, ("col", "band"), to_right)
    ne, wx, cor_u, cor_d = call(
        lambda *a: frame_cols(z, *a), [big, flat, corner, corner], [ne, w, from_r, from_l],
        aliases={0: 0}, flops=cost,
    )
    cor_b = lax.ppermute(cor_u, "row", up)
    cor_a = lax.ppermute(cor_d, "row", down)
    acc = pltpu.VMEM((z.er, 8, z.ec), F32)
    one = pltpu.VMEM(flat, F32)
    ne, wx, qx, qy, s = call(
        lambda *a: frame_rows(z, *a), [big, flat, big, big, flat],
        [kx, ne, wx, ky, below, above, cor_b, cor_a], n_smem=1, aliases={1: 0}, scratch=[acc], flops=20 * cost,
    )
    u = ne
    for k in range(ITERS):
        s = s + lax.ppermute(s, "band", pair_a)
        other = lax.ppermute(s, "band", pair_b)
        if k < ITERS - 1:
            u, qx, qy, s = call(
                lambda *a, k=k: step(z, k, *a), [big, big, big, flat],
                [kx, ne, wx, ky, u, qx, qy, s, other], n_smem=1,
                scratch=[one, acc, acc], flops=20 * cost,
            )
        else:
            keep, send = call(
                lambda *a: last_step(z, ITERS - 1, *a), [(z.r, z.b, z.c)] * 2,
                [core[None], ne, wx, u, qx, qy, s, other], n_smem=1,
                scratch=[one, acc, pltpu.VMEM((z.r, z.nb, z.c), F32)], flops=10 * cost,
            )
    recv = lax.ppermute(send, "band", swap)
    first = jnp.where(core == 0, keep, recv)
    second = jnp.where(core == 0, recv, keep)
    return jnp.swapaxes(jnp.concatenate([first, second], axis=2), 0, 1)


def solution(mesh):
    placed = (P("band", "row", "col"), P("row", "col"))
    return jax.shard_map(
        local, mesh=mesh, in_specs=placed, out_specs=P("band", "row", "col"), check_vma=False
    )
```

```python
import jax
import jax.numpy as jnp
from jax import lax
from jax.experimental import pallas as pl
from jax.experimental.pallas import tpu as pltpu
from jax.sharding import PartitionSpec as P

ITERS = 4
M = ITERS
LANES = 128
SIGMA = 0.35
TAU = 0.35


F32 = jnp.float32
U0, QX0, QY0, NE0 = range(4)
VM = pl.BlockSpec(memory_space=pltpu.VMEM)
SM = pl.BlockSpec(memory_space=pltpu.SMEM)
PARAMS = pltpu.CompilerParams(vmem_limit_bytes=6 * 1024 * 1024)


def call(body, outs, ins, n_smem=0, aliases=None, scratch=(), flops=0):
    return pl.pallas_call(
        body,
        out_shape=[pltpu.VMEM(s, F32) for s in outs],
        in_specs=[SM] * n_smem + [VM] * (len(ins) - n_smem),
        out_specs=[VM] * len(outs),
        scratch_shapes=list(scratch),
        input_output_aliases=aliases or {},
        compiler_params=PARAMS,
        cost_estimate=pl.CostEstimate(flops=flops, bytes_accessed=0, transcendentals=0),
    )(*ins)


def lane_iota(shape):
    return lax.broadcasted_iota(jnp.int32, shape, len(shape) - 1)


class Sizes:
    def __init__(self, bands, rows, cols):
        self.b = bands
        self.nb = 2 * bands
        self.bt = self.nb // 8
        self.r = rows
        self.c = cols // 2
        self.er = rows + 2 * M
        self.ec = self.c + LANES
        self.full = self.b // 8 * 8
        self.rest = self.b - self.full


def pack_lanes(tiles, first, width):
    per = LANES // width
    lane = lane_iota((8, LANES))
    out = []
    for v in range(0, len(tiles), per):
        acc = None
        for p, tile in enumerate(tiles[v : v + per]):
            moved = pltpu.roll(tile, (p * width - first) % LANES, axis=1)
            acc = moved if acc is None else jnp.where(lane // width == p, moved, acc)
        out.append(acc)
    return out


def assemble(z, core, keep, recv, w, edge, ne, col_l, col_r, row_u, row_d):
    f, q = z.full, z.rest
    ft = f // 8

    def join(first, second):
        def put(r, _):
            e = r + M + NE0
            for t in range(ft):
                ne[e, t, :, 0 : z.c] = first[r, 8 * t : 8 * t + 8, :]
                ne[e, ft + t, :, 0 : z.c] = second[r, 8 * t : 8 * t + 8, :]
            ne[e, 2 * ft, 0:q, 0 : z.c] = first[r, f : z.b, :]
            ne[e, 2 * ft, q:8, 0 : z.c] = second[r, f : z.b, :]
            return 0

        lax.fori_loop(0, z.r, put, 0)

    pl.when(core[0] == 0)(lambda: join(keep, recv))
    pl.when(core[0] == 1)(lambda: join(recv, keep))
    last = slice(z.c - LANES, z.c)
    left = [ne[NE0 + M + r, t, :, 0:LANES] for r in range(z.r) for t in range(z.bt)]
    left += [w[8 * t : 8 * t + 8, 0:LANES] for t in range(z.r // 8)]
    right = [ne[NE0 + M + r, t, :, last] for r in range(z.r) for t in range(z.bt)]
    right += [w[8 * t : 8 * t + 8, last] for t in range(z.r // 8)]
    for v, tile in enumerate(pack_lanes(left, 0, M)):
        col_l[v] = tile
    for v, tile in enumerate(pack_lanes(right, LANES - M, M)):
        col_r[v] = tile
    for r in range(M):
        for t in range(z.bt):
            row_u[r * z.bt + t] = ne[NE0 + M + r, t, :, 0 : z.c]
            row_d[r * z.bt + t] = ne[NE0 + z.r + r, t, :, 0 : z.c]
    row_u[M * z.bt] = w[0:8, :]
    row_d[M * z.bt] = w[z.r - 8 : z.r, :]


def frame_cols(z, ne_in, w, from_r, from_l, ne, wx, cor_u, cor_d):
    lane = lane_iota((8, LANES))
    per = LANES // M
    units = z.r * z.bt + z.r // 8
    tiles = []
    for k in range(units):
        v, p = divmod(k, per)
        hi = pltpu.roll(from_r[v], (-p * M) % LANES, axis=1)
        lo = pltpu.roll(from_l[v], (LANES - M - p * M) % LANES, axis=1)
        tiles.append(jnp.where(lane < M, hi, jnp.where(lane >= LANES - M, lo, 0.0)))
    for r in range(z.r):
        for t in range(z.bt):
            ne[NE0 + M + r, t, :, z.c : z.ec] = tiles[r * z.bt + t]
    wx[0:M, :] = jnp.zeros((M, z.ec), F32)
    wx[M + z.r : z.er, :] = jnp.zeros((M, z.ec), F32)
    wx[M : M + z.r, 0 : z.c] = w[...]
    for t in range(z.r // 8):
        wx[M + 8 * t : M + 8 * t + 8, z.c : z.ec] = tiles[z.r * z.bt + t]
    up = tiles[: M * z.bt] + [tiles[z.r * z.bt]]
    down = tiles[(z.r - M) * z.bt : z.r * z.bt] + [tiles[units - 1]]
    for v, tile in enumerate(pack_lanes(up, LANES - M, 2 * M)):
        cor_u[v] = tile
    for v, tile in enumerate(pack_lanes(down, LANES - M, 2 * M)):
        cor_d[v] = tile


def masks(z, edge):
    rows = {M - 1: edge[0:1, :], M + z.r - 1: edge[1:2, :]}
    cut = z.c - LANES
    tail = jnp.broadcast_to(edge[2:3, cut : z.ec], (8, z.ec - cut))

    def across(e, d):
        return d * rows[e] if e in rows else d

    def along(d):
        return jnp.concatenate([d[:, 0:cut], d[:, cut : z.ec] * tail], axis=1)

    return across, along


def message_rows(z, k):
    lo, hi = k, z.er - 1 - k
    return lo, hi - lo + (hi - lo) % 2


def message_shape(z, k):
    return (message_rows(z, k)[1] * (z.c // LANES) + 8, LANES)


def write_message(z, k, acc, sums, msg):
    lo, hi = k, z.er - 1 - k
    first, n = message_rows(z, k)
    sums[...] = jnp.zeros_like(sums)
    for e in range(lo, hi):
        sums[e : e + 1, :] = jnp.sum(acc[e], axis=0, keepdims=True)
    for t in range(z.c // LANES):
        msg[t * n : (t + 1) * n, :] = sums[first : first + n, t * LANES : (t + 1) * LANES]
    halo = [sums[8 * g : 8 * g + 8, z.c : z.ec] for g in range(z.er // 8)]
    msg[n * (z.c // LANES) :, :] = pack_lanes(halo, LANES - M, 2 * M)[0]


def read_scale(z, k, msg_a, msg_b, wx, sums, scale):
    lo, hi = k, z.er - 1 - k
    first, n = message_rows(z, k)
    lane = lane_iota((8, LANES))
    sums[...] = jnp.zeros_like(sums)
    for t in range(z.c // LANES):
        part = slice(t * n, (t + 1) * n)
        sums[first : first + n, t * LANES : (t + 1) * LANES] = msg_a[part, :] + msg_b[part, :]
    packed = msg_a[n * (z.c // LANES) :, :] + msg_b[n * (z.c // LANES) :, :]
    for g in range(z.er // 8):
        got = pltpu.roll(packed, (LANES - M - g * 2 * M) % LANES, axis=1)
        sums[8 * g : 8 * g + 8, z.c : z.ec] = jnp.where((lane < M) | (lane >= LANES - M), got, 0.0)
    w = wx[...]
    sums[...] = w / jnp.maximum(w, jnp.sqrt(1.0 + (SIGMA * SIGMA) * sums[...]))
    for e in range(lo, hi):
        scale[e] = jnp.broadcast_to(sums[e : e + 1, :], (8, z.ec))


def frame_rows(z, ne_in, wx_in, edge, below, above, cor_b, cor_a, ne, wx, qx, qy, msg, acc, sums):
    lane = lane_iota((8, LANES))
    per = LANES // (2 * M)
    units = M * z.bt + 1

    def corner(ref, k):
        v, p = divmod(k, per)
        got = pltpu.roll(ref[v], (LANES - M - p * 2 * M) % LANES, axis=1)
        return jnp.where((lane < M) | (lane >= LANES - M), got, 0.0)

    for r in range(M):
        for t in range(z.bt):
            k = r * z.bt + t
            ne[NE0 + M + z.r + r, t, :, 0 : z.c] = below[k]
            ne[NE0 + M + z.r + r, t, :, z.c : z.ec] = corner(cor_b, k)
            ne[NE0 + r, t, :, 0 : z.c] = above[k]
            ne[NE0 + r, t, :, z.c : z.ec] = corner(cor_a, k)
    wx[...] = wx_in[...]
    wx[M + z.r : z.er, 0 : z.c] = below[units - 1][0:M]
    wx[M + z.r : z.er, z.c : z.ec] = corner(cor_b, units - 1)[0:M]
    wx[0:M, 0 : z.c] = above[units - 1][8 - M : 8]
    wx[0:M, z.c : z.ec] = corner(cor_a, units - 1)[8 - M : 8]
    acc[...] = jnp.zeros_like(acc)
    across, along = masks(z, edge)

    def band_tile(t, _):
        here = ne[NE0, t]
        for e in range(z.er - 1):
            below_row = ne[NE0 + e + 1, t]
            gx = across(e, below_row - here)
            gy = along(pltpu.roll(here, z.ec - 1, axis=1) - here)
            qx[QX0 + e, t] = gx
            qy[QY0 + e, t] = gy
            acc[e] = acc[e] + (gx * gx + gy * gy)
            here = below_row
        return 0

    lax.fori_loop(0, z.bt, band_tile, 0)
    write_message(z, 0, acc, sums, msg)


CARRY = 1.0 / (1.0 + TAU)
GAIN = TAU / (1.0 + TAU)


def step(z, k, ne, wx, edge, u_in, qx_in, qy_in, msg_a, msg_b, u, qx, qy, msg, sums, scale, acc):
    lo, hi = k, z.er - 1 - k
    read_scale(z, k, msg_a, msg_b, wx, sums, scale)
    acc[...] = jnp.zeros_like(acc)
    across, along = masks(z, edge)

    def band_tile(t, _):
        px0 = scale[lo] * qx_in[QX0 + lo, t]
        py0 = ub0 = None
        for e in range(lo + 1, hi):
            sc = scale[e]
            px = sc * qx_in[QX0 + e, t]
            py = sc * qy_in[QY0 + e, t]
            div = (px - px0) + (py - pltpu.roll(py, 1, axis=1))
            if k == 0:
                old = ne[NE0 + e, t]
                new = old + (GAIN * SIGMA) * div
            else:
                old = u_in[U0 + e, t]
                new = (CARRY * old + GAIN * ne[NE0 + e, t]) + (GAIN * SIGMA) * div
            ub = (new - old) + new
            u[U0 + e, t] = new
            if e > lo + 1:
                nx = px0 + across(e - 1, ub - ub0)
                ny = py0 + along(pltpu.roll(ub0, z.ec - 1, axis=1) - ub0)
                qx[QX0 + e - 1, t] = nx
                qy[QY0 + e - 1, t] = ny
                acc[e - 1] = acc[e - 1] + (nx * nx + ny * ny)
            px0, py0, ub0 = px, py, ub
        return 0

    lax.fori_loop(0, z.bt, band_tile, 0)
    write_message(z, k + 1, acc, sums, msg)


def last_step(z, k, core, ne, wx, u_in, qx_in, qy_in, msg_a, msg_b, keep, send, sums, scale, u):
    lo, hi = k, z.er - 1 - k
    read_scale(z, k, msg_a, msg_b, wx, sums, scale)

    def band_tile(t, _):
        px0 = scale[lo] * qx_in[QX0 + lo, t]
        for e in range(lo + 1, hi):
            sc = scale[e]
            px = sc * qx_in[QX0 + e, t]
            py = sc * qy_in[QY0 + e, t]
            div = (px - px0) + (py - pltpu.roll(py, 1, axis=1))
            new = (CARRY * u_in[U0 + e, t] + GAIN * ne[NE0 + e, t]) + (GAIN * SIGMA) * div
            u[e - M, t] = new[:, 0 : z.c]
            px0 = px
        return 0

    lax.fori_loop(0, z.bt, band_tile, 0)
    f, q = z.full, z.rest
    ft = f // 8

    def part(first, second):
        def put(r, _):
            for t in range(ft):
                first[r, 8 * t : 8 * t + 8, :] = u[r, t]
                second[r, 8 * t : 8 * t + 8, :] = u[r, ft + t]
            first[r, f : z.b, :] = u[r, 2 * ft, 0:q, :]
            second[r, f : z.b, :] = u[r, 2 * ft, q:8, :]
            return 0

        lax.fori_loop(0, z.r, put, 0)

    pl.when(core[0] == 0)(lambda: part(keep, send))
    pl.when(core[0] == 1)(lambda: part(send, keep))


def local(noisy, weight_map):
    z = Sizes(*noisy.shape)
    n_row, n_col, n_band = (lax.axis_size(a) for a in ("row", "col", "band"))
    chips = n_band // 2
    core = lax.axis_index("band") % 2
    half = core ^ (lax.axis_index("band") // 2 % 2)
    row0 = lax.axis_index("row") * z.r
    col0 = lax.axis_index("col") * (2 * z.c) + half * z.c

    lane = jnp.arange(z.ec)
    gcol = col0 + jnp.where(lane < z.c + LANES // 2, lane, lane - z.ec)
    inner = (gcol >= 0) & (gcol < n_col * 2 * z.c - 1)
    edge = jnp.stack([
        jnp.broadcast_to(row0 > 0, (z.ec,)), jnp.broadcast_to(row0 + z.r < n_row * z.r, (z.ec,)), inner,
    ] + [inner] * 5).astype(F32)

    def at(chip, h):
        return 2 * chip + (h ^ (chip % 2))

    swap = [(i, i ^ 1) for i in range(n_band)]
    pair_a = [(at(c, h), at(c ^ 1, h)) for c in range(chips) for h in range(2)]
    pair_b = [(at(c, h), at((c - 1 + 2 * (c % 2)) % chips, h)) for c in range(chips) for h in range(2)]
    up = [((i + 1) % n_row, i) for i in range(n_row)]
    down = [(i, (i + 1) % n_row) for i in range(n_row)]
    spot = [[(j // 2) * n_band + at(c, j % 2) for j in range(2 * n_col)] for c in range(chips)]
    to_right = [(line[j], line[(j + 1) % len(line)]) for line in spot for j in range(len(line))]
    to_left = [(b, a) for a, b in to_right]

    turned = jnp.swapaxes(noisy, 0, 1)
    keep = lax.dynamic_slice_in_dim(turned, half * z.c, z.c, axis=2)
    send = lax.dynamic_slice_in_dim(turned, (1 - half) * z.c, z.c, axis=2)
    w = lax.dynamic_slice_in_dim(weight_map, half * z.c, z.c, axis=1)
    recv = lax.ppermute(send, "band", swap)

    units = z.r * z.bt + z.r // 8
    n_edge = -(-units // (LANES // M))
    n_corner = -(-(M * z.bt + 1) // (LANES // (2 * M)))
    state = (z.er + 4, z.bt, 8, z.ec)
    flat = (z.er, z.ec)
    side = (n_edge, 8, LANES)
    bulk = (M * z.bt + 1, 8, z.c)
    corner = (n_corner, 8, LANES)
    cost = z.er * z.nb * z.ec

    ne, col_l, col_r, row_u, row_d = call(
        lambda *a: assemble(z, *a), [state, side, side, bulk, bulk], [core[None], keep, recv, w, edge],
        n_smem=1, flops=cost,
    )
    below = lax.ppermute(row_u, "row", up)
    above = lax.ppermute(row_d, "row", down)
    from_r = lax.ppermute(col_l, ("col", "band"), to_left)
    from_l = lax.ppermute(col_r, ("col", "band"), to_right)
    ne, wx, cor_u, cor_d = call(
        lambda *a: frame_cols(z, *a), [state, flat, corner, corner], [ne, w, from_r, from_l],
        aliases={0: 0}, flops=cost,
    )
    cor_b = lax.ppermute(cor_u, "row", up)
    cor_a = lax.ppermute(cor_d, "row", down)
    acc = pltpu.VMEM((z.er, 8, z.ec), F32)
    one = pltpu.VMEM(flat, F32)
    ne, wx, qx, qy, msg = call(
        lambda *a: frame_rows(z, *a), [state, flat, state, state, message_shape(z, 0)],
        [ne, wx, edge, below, above, cor_b, cor_a], aliases={0: 0}, scratch=[acc, one], flops=20 * cost,
    )
    u = ne
    for k in range(ITERS):
        msg = msg + lax.ppermute(msg, "band", pair_a)
        other = lax.ppermute(msg, "band", pair_b)
        if k < ITERS - 1:
            u, qx, qy, msg = call(
                lambda *a, k=k: step(z, k, *a), [state, state, state, message_shape(z, k + 1)],
                [ne, wx, edge, u, qx, qy, msg, other], scratch=[one, acc, acc], flops=20 * cost,
            )
        else:
            keep, send = call(
                lambda *a: last_step(z, ITERS - 1, *a), [(z.r, z.b, z.c)] * 2,
                [core[None], ne, wx, u, qx, qy, msg, other], n_smem=1,
                scratch=[one, acc, pltpu.VMEM((z.r, z.bt, 8, z.c), F32)], flops=10 * cost,
            )
    recv = lax.ppermute(send, "band", swap)
    first = jnp.where(half == 0, keep, recv)
    second = jnp.where(half == 0, recv, keep)
    return jnp.swapaxes(jnp.concatenate([first, second], axis=2), 0, 1)


def solution(mesh):
    placed = (P("band", "row", "col"), P("row", "col"))
    return jax.shard_map(
        local, mesh=mesh, in_specs=placed, out_specs=P("band", "row", "col"), check_vma=False
    )
```

```python
import jax
import jax.numpy as jnp
from jax import lax
from jax.experimental import pallas as pl
from jax.experimental.pallas import tpu as pltpu
from jax.sharding import PartitionSpec as P

ITERS = 4
M = ITERS
LANES = 128
SIGMA = 0.35
TAU = 0.35


F32 = jnp.float32
U0, QX0, QY0, NE0 = range(4)
VM = pl.BlockSpec(memory_space=pltpu.VMEM)
SM = pl.BlockSpec(memory_space=pltpu.SMEM)
HB = pl.BlockSpec(memory_space=pltpu.HBM)
PARAMS = pltpu.CompilerParams(vmem_limit_bytes=6 * 1024 * 1024)


def call(body, outs, ins, n_smem=0, aliases=None, scratch=(), flops=0, hbm_in=(), hbm_out=()):
    in_specs = [SM] * n_smem + [VM] * (len(ins) - n_smem)
    return pl.pallas_call(
        body,
        out_shape=[(pltpu.HBM if i in hbm_out else pltpu.VMEM)(s, F32) for i, s in enumerate(outs)],
        in_specs=[HB if i in hbm_in else spec for i, spec in enumerate(in_specs)],
        out_specs=[HB if i in hbm_out else VM for i in range(len(outs))],
        scratch_shapes=list(scratch),
        input_output_aliases=aliases or {},
        compiler_params=PARAMS,
        cost_estimate=pl.CostEstimate(flops=flops, bytes_accessed=0, transcendentals=0),
    )(*ins)


def lane_iota(shape):
    return lax.broadcasted_iota(jnp.int32, shape, len(shape) - 1)


class Sizes:
    def __init__(self, bands, rows, cols):
        self.b = bands
        self.nb = 2 * bands
        self.bt = self.nb // 8
        self.r = rows
        self.c = cols // 2
        self.er = rows + 2 * M
        self.ec = self.c + LANES
        self.full = self.b // 8 * 8
        self.rest = self.b - self.full
        self.ft = self.full // 8
        self.rg = rows // 8
        self.lt = self.c // LANES
        self.block = (self.rg, self.lt, self.b, 8, LANES)


def pack_lanes(tiles, first, width):
    per = LANES // width
    lane = lane_iota((8, LANES))
    out = []
    for v in range(0, len(tiles), per):
        acc = None
        for p, tile in enumerate(tiles[v : v + per]):
            moved = pltpu.roll(tile, (p * width - first) % LANES, axis=1)
            acc = moved if acc is None else jnp.where(lane // width == p, moved, acc)
        out.append(acc)
    return out


def flat_rows(ref, g, t):
    tile = ref.at[g, t]
    return tile.reshape(tile.shape[0] * 8, LANES)


def half_copies(z, half, array, block, sem, out=False):
    copies = []
    for g in range(z.rg):
        for t in range(z.lt):
            lanes = pl.ds(pl.multiple_of(half * z.c + t * LANES, LANES), LANES)
            ends = [array.at[:, pl.ds(8 * g, 8), lanes], block.at[g, t]]
            copies.append(pltpu.make_async_copy(*(ends[::-1] if out else ends), sem.at[g * z.lt + t]))
    return copies


def split(z, place, noisy, keep, send, a_keep, a_send, b_keep, b_send, sem_k, sem_s):
    half, odd = place[1], place[2]
    copies = half_copies(z, half, noisy, keep, sem_k) + half_copies(z, 1 - half, noisy, send, sem_s)
    for c in copies:
        c.start()
    for c in copies:
        c.wait()

    def rows(block, first, msg):
        for i in range(M):
            g, q = divmod(first + i, 8)
            for t in range(z.lt):
                run = flat_rows(block, g, t)
                lanes = slice(t * LANES, (t + 1) * LANES)
                for bt in range(z.ft):
                    msg[z.ft * i + bt, :, lanes] = run[pl.ds(64 * bt + q, 8, stride=8), :]
                at = z.rest * (i % 2)
                msg[z.ft * M + i // 2, at : at + z.rest, lanes] = run[pl.ds(8 * z.full + q, z.rest, stride=8), :]

    @pl.when(odd == 0)
    def _():
        rows(keep, z.r - M, a_keep)
        rows(send, z.r - M, a_send)
        rows(keep, 0, b_keep)
        rows(send, 0, b_send)

    @pl.when(odd == 1)
    def _():
        rows(keep, 0, a_keep)
        rows(send, 0, a_send)
        rows(keep, z.r - M, b_keep)
        rows(send, z.r - M, b_send)


def half_of(z, place, w):
    return jnp.where(place[1] == 0, w[:, 0 : z.c], w[:, z.c : 2 * z.c])


def assemble(z, place, keep, recv, w_whole, edge, ne, col_l, col_r):
    core = place[0]
    w = half_of(z, place, w_whole)
    q4 = z.rest
    for r in range(z.r):
        g, q = divmod(r, 8)
        for t in range(z.lt):
            lanes = slice(t * LANES, (t + 1) * LANES)
            mine, other = flat_rows(keep, g, t), flat_rows(recv, g, t)
            for bt in range(z.ft):
                ne[NE0 + M + r, core * z.ft + bt, :, lanes] = mine[pl.ds(64 * bt + q, 8, stride=8), :]
                ne[NE0 + M + r, (1 - core) * z.ft + bt, :, lanes] = other[pl.ds(64 * bt + q, 8, stride=8), :]
            a = mine[pl.ds(8 * z.full + q, q4, stride=8), :]
            b = other[pl.ds(8 * z.full + q, q4, stride=8), :]
            ne[NE0 + M + r, 2 * z.ft, 0:q4, lanes] = jnp.where(core == 0, a, b)
            ne[NE0 + M + r, 2 * z.ft, q4:8, lanes] = jnp.where(core == 0, b, a)
    last = slice(z.c - LANES, z.c)
    left = [ne[NE0 + M + r, t, :, 0:LANES] for r in range(z.r) for t in range(z.bt)]
    left += [w[8 * t : 8 * t + 8, 0:LANES] for t in range(z.r // 8)]
    right = [ne[NE0 + M + r, t, :, last] for r in range(z.r) for t in range(z.bt)]
    right += [w[8 * t : 8 * t + 8, last] for t in range(z.r // 8)]
    for v, tile in enumerate(pack_lanes(left, 0, M)):
        col_l[v] = tile
    for v, tile in enumerate(pack_lanes(right, LANES - M, M)):
        col_r[v] = tile


def frame_cols(z, place, ne_in, w_whole, from_r, from_l, ne, wx, cor_a, cor_b):
    w = half_of(z, place, w_whole)
    lane = lane_iota((8, LANES))
    per = LANES // M
    units = z.r * z.bt + z.r // 8
    tiles = []
    for k in range(units):
        v, p = divmod(k, per)
        hi = pltpu.roll(from_r[v], (-p * M) % LANES, axis=1)
        lo = pltpu.roll(from_l[v], (LANES - M - p * M) % LANES, axis=1)
        tiles.append(jnp.where(lane < M, hi, jnp.where(lane >= LANES - M, lo, 0.0)))
    for r in range(z.r):
        for t in range(z.bt):
            ne[NE0 + M + r, t, :, z.c : z.ec] = tiles[r * z.bt + t]
    wx[0:M, :] = jnp.zeros((M, z.ec), F32)
    wx[M + z.r : z.er, :] = jnp.zeros((M, z.ec), F32)
    wx[M : M + z.r, 0 : z.c] = w
    for t in range(z.r // 8):
        wx[M + 8 * t : M + 8 * t + 8, z.c : z.ec] = tiles[z.r * z.bt + t]
    up = tiles[: M * z.bt] + [tiles[z.r * z.bt]]
    down = tiles[(z.r - M) * z.bt : z.r * z.bt] + [tiles[units - 1]]
    up, down = (pack_lanes(x, LANES - M, 2 * M) for x in (up, down))
    lanes = [slice(t * LANES, (t + 1) * LANES) for t in range(z.lt)]
    up += [w[0:8, x] for x in lanes]
    down += [w[z.r - 8 : z.r, x] for x in lanes]
    odd = place[2]
    for v, (u, d) in enumerate(zip(up, down)):
        cor_a[v] = jnp.where(odd == 0, d, u)
        cor_b[v] = jnp.where(odd == 0, u, d)


def masks(z, edge):
    rows = {M - 1: edge[0:1, :], M + z.r - 1: edge[1:2, :]}
    cut = z.c - LANES
    tail = jnp.broadcast_to(edge[2:3, cut : z.ec], (8, z.ec - cut))

    def across(e, d):
        return d * rows[e] if e in rows else d

    def along(d):
        return jnp.concatenate([d[:, 0:cut], d[:, cut : z.ec] * tail], axis=1)

    return across, along


def message_rows(z, k):
    lo, hi = k, z.er - 1 - k
    return lo, hi - lo + (hi - lo) % 2


def message_shape(z, k):
    return (message_rows(z, k)[1] * (z.c // LANES) + 8, LANES)


def write_message(z, k, acc, sums, msg):
    lo, hi = k, z.er - 1 - k
    first, n = message_rows(z, k)
    sums[...] = jnp.zeros_like(sums)
    for e in range(lo, hi):
        sums[e : e + 1, :] = jnp.sum(acc[e], axis=0, keepdims=True)
    for t in range(z.c // LANES):
        msg[t * n : (t + 1) * n, :] = sums[first : first + n, t * LANES : (t + 1) * LANES]
    halo = [sums[8 * g : 8 * g + 8, z.c : z.ec] for g in range(z.er // 8)]
    msg[n * (z.c // LANES) :, :] = pack_lanes(halo, LANES - M, 2 * M)[0]


def read_scale(z, k, msg_a, msg_b, wx, sums, scale):
    lo, hi = k, z.er - 1 - k
    first, n = message_rows(z, k)
    lane = lane_iota((8, LANES))
    sums[...] = jnp.zeros_like(sums)
    for t in range(z.c // LANES):
        part = slice(t * n, (t + 1) * n)
        sums[first : first + n, t * LANES : (t + 1) * LANES] = msg_a[part, :] + msg_b[part, :]
    packed = msg_a[n * (z.c // LANES) :, :] + msg_b[n * (z.c // LANES) :, :]
    for g in range(z.er // 8):
        got = pltpu.roll(packed, (LANES - M - g * 2 * M) % LANES, axis=1)
        sums[8 * g : 8 * g + 8, z.c : z.ec] = jnp.where((lane < M) | (lane >= LANES - M), got, 0.0)
    w = wx[...]
    sums[...] = w / jnp.maximum(w, jnp.sqrt(1.0 + (SIGMA * SIGMA) * sums[...]))
    for e in range(lo, hi):
        scale[e] = jnp.broadcast_to(sums[e : e + 1, :], (8, z.ec))


def frame_rows(z, place, ne_in, wx_in, edge, a_keep, a_send, b_keep, b_send, cor_a, cor_b, ne, wx, qx, qy, msg, acc, sums):
    core, odd = place[0], place[2]
    lane = lane_iota((8, LANES))
    sub = lax.broadcasted_iota(jnp.int32, (8, z.c), 0)
    per = LANES // (2 * M)
    q4 = z.rest

    for keep, send, first in ((a_keep, a_send, (1 - odd) * (M + z.r)), (b_keep, b_send, odd * (M + z.r))):
        for i in range(M):
            e = NE0 + first + i
            for bt in range(z.ft):
                ne[e, core * z.ft + bt, :, 0 : z.c] = keep[z.ft * i + bt]
                ne[e, (1 - core) * z.ft + bt, :, 0 : z.c] = send[z.ft * i + bt]
            k, s = keep[z.ft * M + i // 2], send[z.ft * M + i // 2]
            k0, s0 = jnp.where(core == 0, k, s), jnp.where(core == 0, s, k)
            if i % 2 == 0:
                s0 = pltpu.roll(s0, q4, axis=0)
            else:
                k0 = pltpu.roll(k0, q4, axis=0)
            ne[e, 2 * z.ft, :, 0 : z.c] = jnp.where(sub < q4, k0, s0)

    n_cor = cor_a.shape[0] - z.lt
    below = [jnp.where(odd == 0, cor_a[v], cor_b[v]) for v in range(n_cor + z.lt)]
    above = [jnp.where(odd == 0, cor_b[v], cor_a[v]) for v in range(n_cor + z.lt)]

    def corner(got, k):
        v, p = divmod(k, per)
        moved = pltpu.roll(got[v], (LANES - M - p * 2 * M) % LANES, axis=1)
        return jnp.where((lane < M) | (lane >= LANES - M), moved, 0.0)

    for r in range(M):
        for t in range(z.bt):
            ne[NE0 + M + z.r + r, t, :, z.c : z.ec] = corner(below, r * z.bt + t)
            ne[NE0 + r, t, :, z.c : z.ec] = corner(above, r * z.bt + t)
    wx[...] = wx_in[...]
    for t in range(z.lt):
        lanes = slice(t * LANES, (t + 1) * LANES)
        wx[M + z.r : z.er, lanes] = below[n_cor + t][0:M]
        wx[0:M, lanes] = above[n_cor + t][8 - M : 8]
    wx[M + z.r : z.er, z.c : z.ec] = corner(below, M * z.bt)[0:M]
    wx[0:M, z.c : z.ec] = corner(above, M * z.bt)[8 - M : 8]
    acc[...] = jnp.zeros_like(acc)
    across, along = masks(z, edge)

    def band_tile(t, _):
        here = ne[NE0, t]
        for e in range(z.er - 1):
            below_row = ne[NE0 + e + 1, t]
            gx = across(e, below_row - here)
            gy = along(pltpu.roll(here, z.ec - 1, axis=1) - here)
            qx[QX0 + e, t] = gx
            qy[QY0 + e, t] = gy
            acc[e] = acc[e] + (gx * gx + gy * gy)
            here = below_row
        return 0

    lax.fori_loop(0, z.bt, band_tile, 0)
    write_message(z, 0, acc, sums, msg)


CARRY = 1.0 / (1.0 + TAU)
GAIN = TAU / (1.0 + TAU)


def step(z, k, ne, wx, edge, u_in, qx_in, qy_in, msg_a, msg_b, u, qx, qy, msg, sums, scale, acc, ubs):
    lo, hi = k, z.er - 1 - k
    read_scale(z, k, msg_a, msg_b, wx, sums, scale)
    acc[...] = jnp.zeros_like(acc)
    across, along = masks(z, edge)

    def band_tile(t, _):
        px0 = scale[lo] * qx_in[QX0 + lo, t]
        for e in range(lo + 1, hi):
            sc = scale[e]
            px = sc * qx_in[QX0 + e, t]
            py = sc * qy_in[QY0 + e, t]
            div = ((px - px0) + py) - pltpu.roll(py, 1, axis=1)
            if k == 0:
                old = ne[NE0 + e, t]
                new = old + (GAIN * SIGMA) * div
            else:
                old = u_in[U0 + e, t]
                new = (CARRY * old + GAIN * ne[NE0 + e, t]) + (GAIN * SIGMA) * div
            u[U0 + e, t] = new
            ubs[e] = (new - old) + new
            px0 = px
        ub0 = ubs[lo + 1]
        for e in range(lo + 1, hi - 1):
            sc = scale[e]
            ub = ubs[e + 1]
            nx = sc * qx_in[QX0 + e, t] + across(e, ub - ub0)
            ny = sc * qy_in[QY0 + e, t] + along(pltpu.roll(ub0, z.ec - 1, axis=1) - ub0)
            qx[QX0 + e, t] = nx
            qy[QY0 + e, t] = ny
            acc[e] = acc[e] + (nx * nx + ny * ny)
            ub0 = ub
        return 0

    lax.fori_loop(0, z.bt, band_tile, 0)
    write_message(z, k + 1, acc, sums, msg)


def last_step(z, k, place, ne, wx, u_in, qx_in, qy_in, msg_a, msg_b, keep, send, sums, scale, u):
    lo, hi = k, z.er - 1 - k
    read_scale(z, k, msg_a, msg_b, wx, sums, scale)

    def band_tile(t, _):
        px0 = scale[lo] * qx_in[QX0 + lo, t]
        for e in range(lo + 1, hi):
            sc = scale[e]
            px = sc * qx_in[QX0 + e, t]
            py = sc * qy_in[QY0 + e, t]
            div = (px - px0) + (py - pltpu.roll(py, 1, axis=1))
            new = (CARRY * u_in[U0 + e, t] + GAIN * ne[NE0 + e, t]) + (GAIN * SIGMA) * div
            u[e - M, t] = new[:, 0 : z.c]
            px0 = px
        return 0

    lax.fori_loop(0, z.bt, band_tile, 0)
    core = place[0]
    q4 = z.rest
    for r in range(z.r):
        g, q = divmod(r, 8)
        for t in range(z.lt):
            lanes = slice(t * LANES, (t + 1) * LANES)
            mine, other = flat_rows(keep, g, t), flat_rows(send, g, t)
            for bt in range(z.ft):
                mine[pl.ds(64 * bt + q, 8, stride=8), :] = u[r, core * z.ft + bt, :, lanes]
                other[pl.ds(64 * bt + q, 8, stride=8), :] = u[r, (1 - core) * z.ft + bt, :, lanes]
            a, b = u[r, 2 * z.ft, 0:q4, lanes], u[r, 2 * z.ft, q4:8, lanes]
            mine[pl.ds(8 * z.full + q, q4, stride=8), :] = jnp.where(core == 0, a, b)
            other[pl.ds(8 * z.full + q, q4, stride=8), :] = jnp.where(core == 0, b, a)


def write_half(z, own, place, block, *refs):
    out, sem = refs[-2:]
    copies = half_copies(z, place[1] if own else 1 - place[1], out, block, sem, out=True)
    for c in copies:
        c.start()
    for c in copies:
        c.wait()


def local(noisy, weight_map):
    z = Sizes(*noisy.shape)
    n_row, n_col, n_band = (lax.axis_size(a) for a in ("row", "col", "band"))
    chips = n_band // 2
    core = lax.axis_index("band") % 2
    half = core ^ (lax.axis_index("band") // 2 % 2)
    row0 = lax.axis_index("row") * z.r
    col0 = lax.axis_index("col") * (2 * z.c) + half * z.c

    lane = jnp.arange(z.ec)
    gcol = col0 + jnp.where(lane < z.c + LANES // 2, lane, lane - z.ec)
    inner = (gcol >= 0) & (gcol < n_col * 2 * z.c - 1)
    edge = jnp.stack([
        jnp.broadcast_to(row0 > 0, (z.ec,)), jnp.broadcast_to(row0 + z.r < n_row * z.r, (z.ec,)), inner,
    ] + [inner] * 5).astype(F32)

    def at(chip, h):
        return 2 * chip + (h ^ (chip % 2))

    swap = [(i, i ^ 1) for i in range(n_band)]
    pair_a = [(at(c, h), at(c ^ 1, h)) for c in range(chips) for h in range(2)]
    pair_b = [(at(c, h), at((c - 1 + 2 * (c % 2)) % chips, h)) for c in range(chips) for h in range(2)]
    rows_a = [(i, i ^ 1) for i in range(n_row)]
    rows_b = [(i, min(max(i - 1 + 2 * (i % 2), 0), n_row - 1)) for i in range(n_row)]
    across_a = [(i * n_band + b, j * n_band + (b ^ 1)) for i, j in rows_a for b in range(n_band)]
    across_b = [(i * n_band + b, j * n_band + (b ^ 1)) for i, j in rows_b for b in range(n_band)]
    spot = [[(j // 2) * n_band + at(c, j % 2) for j in range(2 * n_col)] for c in range(chips)]
    to_right = [(line[j], line[(j + 1) % len(line)]) for line in spot for j in range(len(line))]
    to_left = [(b, a) for a, b in to_right]

    odd = lax.axis_index("row") % 2
    place = jnp.stack([core, half, odd]).astype(jnp.int32)
    place, edge = lax.optimization_barrier((place, edge))
    w = weight_map

    units = z.r * z.bt + z.r // 8
    n_edge = -(-units // (LANES // M))
    n_corner = -(-(M * z.bt + 1) // (LANES // (2 * M)))
    state = (z.er + 4, z.bt, 8, z.ec)
    flat = (z.er, z.ec)
    side = (n_edge, 8, LANES)
    bulk = (z.ft * M + M * z.rest // 8, 8, z.c)
    corner = (n_corner + z.lt, 8, LANES)
    cost = z.er * z.nb * z.ec
    sem = pltpu.SemaphoreType.DMA((z.rg * z.lt,))

    keep, send, a_keep, a_send, b_keep, b_send = call(
        lambda *a: split(z, *a), [z.block, z.block] + [bulk] * 4, [place, pltpu.with_memory_space_constraint(noisy, pltpu.HBM)],
        n_smem=1, scratch=[sem, sem], hbm_in=(1,), flops=cost,
    )
    a_keep = lax.ppermute(a_keep, "row", rows_a)
    a_send = lax.ppermute(a_send, ("row", "band"), across_a)
    b_keep = lax.ppermute(b_keep, "row", rows_b)
    b_send = lax.ppermute(b_send, ("row", "band"), across_b)
    recv = lax.ppermute(send, "band", swap)
    ne, col_l, col_r = call(
        lambda *a: assemble(z, *a), [state, side, side], [place, keep, recv, w, edge], n_smem=1, flops=cost
    )
    from_r = lax.ppermute(col_l, ("col", "band"), to_left)
    from_l = lax.ppermute(col_r, ("col", "band"), to_right)
    ne, wx, cor_a, cor_b = call(
        lambda *a: frame_cols(z, *a), [state, flat, corner, corner], [place, ne, w, from_r, from_l],
        n_smem=1, aliases={1: 0}, flops=cost,
    )
    cor_a = lax.ppermute(cor_a, "row", rows_a)
    cor_b = lax.ppermute(cor_b, "row", rows_b)
    acc = pltpu.VMEM((z.er, 8, z.ec), F32)
    one = pltpu.VMEM(flat, F32)
    ne, wx, qx, qy, msg = call(
        lambda *a: frame_rows(z, *a), [state, flat, state, state, message_shape(z, 0)],
        [place, ne, wx, edge, a_keep, a_send, b_keep, b_send, cor_a, cor_b],
        n_smem=1, aliases={1: 0}, scratch=[acc, one], flops=20 * cost,
    )
    u = ne
    for k in range(ITERS):
        msg = msg + lax.ppermute(msg, "band", pair_a)
        other = lax.ppermute(msg, "band", pair_b)
        if k < ITERS - 1:
            u, qx, qy, msg = call(
                lambda *a, k=k: step(z, k, *a), [state, state, state, message_shape(z, k + 1)],
                [ne, wx, edge, u, qx, qy, msg, other], scratch=[one, acc, acc, acc], flops=20 * cost,
            )
        else:
            keep, send = call(
                lambda *a: last_step(z, ITERS - 1, *a), [z.block, z.block],
                [place, ne, wx, u, qx, qy, msg, other], n_smem=1,
                scratch=[one, acc, pltpu.VMEM((z.r, z.bt, 8, z.c), F32)], flops=10 * cost,
            )
    recv = lax.ppermute(send, "band", swap)
    (out,) = call(
        lambda *a: write_half(z, True, *a), [noisy.shape], [place, keep],
        n_smem=1, scratch=[sem], hbm_out=(0,), flops=cost,
    )
    (out,) = call(
        lambda *a: write_half(z, False, *a), [noisy.shape], [place, recv, out],
        n_smem=1, aliases={2: 0}, scratch=[sem], hbm_in=(2,), hbm_out=(0,), flops=cost,
    )
    return out


def solution(mesh):
    placed = (P("band", "row", "col"), P("row", "col"))
    return jax.shard_map(
        local, mesh=mesh, in_specs=placed, out_specs=P("band", "row", "col"), check_vma=False
    )
```

```python
import jax
import jax.numpy as jnp
from jax import lax
from jax.experimental import pallas as pl
from jax.experimental.pallas import tpu as pltpu
from jax.sharding import PartitionSpec as P

ITERS = 4
M = ITERS
LANES = 128
SIGMA = 0.35
TAU = 0.35


F32 = jnp.float32
U0, QX0, QY0, NE0 = range(4)
VM = pl.BlockSpec(memory_space=pltpu.VMEM)
SM = pl.BlockSpec(memory_space=pltpu.SMEM)
HB = pl.BlockSpec(memory_space=pltpu.HBM)
PARAMS = pltpu.CompilerParams(vmem_limit_bytes=6 * 1024 * 1024)


def call(body, outs, ins, n_smem=0, aliases=None, scratch=(), flops=0, hbm_in=(), hbm_out=()):
    in_specs = [SM] * n_smem + [VM] * (len(ins) - n_smem)
    return pl.pallas_call(
        body,
        out_shape=[(pltpu.HBM if i in hbm_out else pltpu.VMEM)(s, F32) for i, s in enumerate(outs)],
        in_specs=[HB if i in hbm_in else spec for i, spec in enumerate(in_specs)],
        out_specs=[HB if i in hbm_out else VM for i in range(len(outs))],
        scratch_shapes=list(scratch),
        input_output_aliases=aliases or {},
        compiler_params=PARAMS,
        cost_estimate=pl.CostEstimate(flops=flops, bytes_accessed=0, transcendentals=0),
    )(*ins)


def lane_iota(shape):
    return lax.broadcasted_iota(jnp.int32, shape, len(shape) - 1)


class Sizes:
    def __init__(self, bands, rows, cols):
        self.b = bands
        self.nb = 2 * bands
        self.bt = self.nb // 8
        self.r = rows
        self.c = cols // 2
        self.er = rows + 2 * M
        self.ec = self.c + LANES
        self.full = self.b // 8 * 8
        self.rest = self.b - self.full
        self.ft = self.full // 8
        self.rg = rows // 8
        self.lt = self.c // LANES
        self.block = (self.rg, self.lt, self.b, 8, LANES)


def pack_lanes(tiles, first, width):
    per = LANES // width
    lane = lane_iota((8, LANES))
    out = []
    for v in range(0, len(tiles), per):
        acc = None
        for p, tile in enumerate(tiles[v : v + per]):
            moved = pltpu.roll(tile, (p * width - first) % LANES, axis=1)
            acc = moved if acc is None else jnp.where(lane // width == p, moved, acc)
        out.append(acc)
    return out


def flat_rows(ref, *at):
    tile = ref.at[at]
    return tile.reshape(tile.shape[0] * 8, LANES)


def half_copies(z, half, array, block, sem, out=False):
    copies = []
    for g in range(z.rg):
        for t in range(z.lt):
            lanes = pl.ds(pl.multiple_of(half * z.c + t * LANES, LANES), LANES)
            ends = [array.at[:, pl.ds(8 * g, 8), lanes], block.at[g, t]]
            copies.append(pltpu.make_async_copy(*(ends[::-1] if out else ends), sem.at[g * z.lt + t]))
    return copies


def split(z, place, noisy, keep, send, a_keep, a_send, b_keep, b_send, sem_k, sem_s):
    half, odd = place[1], place[2]
    kept, sent = half_copies(z, half, noisy, keep, sem_k), half_copies(z, 1 - half, noisy, send, sem_s)
    groups = [kept[g * z.lt : (g + 1) * z.lt] + sent[g * z.lt : (g + 1) * z.lt] for g in range(z.rg)]
    for c in sum(groups, []):
        c.start()

    def rows(block, first, msg):
        for i in range(M):
            g, q = divmod(first + i, 8)
            for t in range(z.lt):
                run = flat_rows(block, g, t)
                lanes = slice(t * LANES, (t + 1) * LANES)
                for bt in range(z.ft):
                    msg[z.ft * i + bt, :, lanes] = run[pl.ds(64 * bt + q, 8, stride=8), :]
                at = z.rest * (i % 2)
                msg[z.ft * M + i // 2, at : at + z.rest, lanes] = run[pl.ds(8 * z.full + q, z.rest, stride=8), :]

    def gather(first, even, other):
        @pl.when(odd == 0)
        def _():
            rows(keep, first, even[0])
            rows(send, first, even[1])

        @pl.when(odd == 1)
        def _():
            rows(keep, first, other[0])
            rows(send, first, other[1])

    for n, copies in enumerate(groups):
        for c in copies:
            c.wait()
        if n == 0:
            gather(0, (b_keep, b_send), (a_keep, a_send))
        if n == z.rg - 1:
            gather(z.r - M, (a_keep, a_send), (b_keep, b_send))


def half_of(z, place, w):
    return jnp.where(place[1] == 0, w[:, 0 : z.c], w[:, z.c : 2 * z.c])


def assemble(z, place, keep, recv, w_whole, edge, ne, col_l, col_r):
    core = place[0]
    w = half_of(z, place, w_whole)
    q4 = z.rest
    for r in range(z.r):
        g, q = divmod(r, 8)
        for t in range(z.lt):
            lanes = slice(t * LANES, (t + 1) * LANES)
            mine, other = flat_rows(keep, g, t), flat_rows(recv, g, t)
            for bt in range(z.ft):
                ne[NE0 + M + r, core * z.ft + bt, :, lanes] = mine[pl.ds(64 * bt + q, 8, stride=8), :]
                ne[NE0 + M + r, (1 - core) * z.ft + bt, :, lanes] = other[pl.ds(64 * bt + q, 8, stride=8), :]
            a = mine[pl.ds(8 * z.full + q, q4, stride=8), :]
            b = other[pl.ds(8 * z.full + q, q4, stride=8), :]
            ne[NE0 + M + r, 2 * z.ft, 0:q4, lanes] = jnp.where(core == 0, a, b)
            ne[NE0 + M + r, 2 * z.ft, q4:8, lanes] = jnp.where(core == 0, b, a)
    last = slice(z.c - LANES, z.c)
    left = [ne[NE0 + M + r, t, :, 0:LANES] for r in range(z.r) for t in range(z.bt)]
    left += [w[8 * t : 8 * t + 8, 0:LANES] for t in range(z.r // 8)]
    right = [ne[NE0 + M + r, t, :, last] for r in range(z.r) for t in range(z.bt)]
    right += [w[8 * t : 8 * t + 8, last] for t in range(z.r // 8)]
    for v, tile in enumerate(pack_lanes(left, 0, M)):
        col_l[v] = tile
    for v, tile in enumerate(pack_lanes(right, LANES - M, M)):
        col_r[v] = tile


def frame_cols(z, place, ne_in, w_whole, edge, from_r, from_l, ne, wx, qx, qy, sums, cor_a, cor_b, acc):
    w = half_of(z, place, w_whole)
    lane = lane_iota((8, LANES))
    per = LANES // M
    units = z.r * z.bt + z.r // 8
    tiles = []
    for k in range(units):
        v, p = divmod(k, per)
        hi = pltpu.roll(from_r[v], (-p * M) % LANES, axis=1)
        lo = pltpu.roll(from_l[v], (LANES - M - p * M) % LANES, axis=1)
        tiles.append(jnp.where(lane < M, hi, jnp.where(lane >= LANES - M, lo, 0.0)))
    for r in range(z.r):
        for t in range(z.bt):
            ne[NE0 + M + r, t, :, z.c : z.ec] = tiles[r * z.bt + t]
    wx[0:M, :] = jnp.zeros((M, z.ec), F32)
    wx[M + z.r : z.er, :] = jnp.zeros((M, z.ec), F32)
    wx[M : M + z.r, 0 : z.c] = w
    for t in range(z.r // 8):
        wx[M + 8 * t : M + 8 * t + 8, z.c : z.ec] = tiles[z.r * z.bt + t]
    up = tiles[: M * z.bt] + [tiles[z.r * z.bt]]
    down = tiles[(z.r - M) * z.bt : z.r * z.bt] + [tiles[units - 1]]
    up, down = (pack_lanes(x, LANES - M, 2 * M) for x in (up, down))
    lanes = [slice(t * LANES, (t + 1) * LANES) for t in range(z.lt)]
    up += [w[0:8, x] for x in lanes]
    down += [w[z.r - 8 : z.r, x] for x in lanes]
    odd = place[2]
    for v, (u, d) in enumerate(zip(up, down)):
        cor_a[v] = jnp.where(odd == 0, d, u)
        cor_b[v] = jnp.where(odd == 0, u, d)
    sums[...] = jnp.zeros_like(sums)
    first_q(z, ne, edge, [(M, M + z.r - 1)], qx, qy, acc, sums)


def first_q(z, ne, edge, runs, qx, qy, acc, sums):
    across, along = masks(z, edge)
    acc[...] = jnp.zeros_like(acc)

    def band_tile(t, _):
        for lo, hi in runs:
            here = ne[NE0 + lo, t]
            for e in range(lo, hi):
                below_row = ne[NE0 + e + 1, t]
                gx = across(e, below_row - here)
                gy = along(pltpu.roll(here, z.ec - 1, axis=1) - here)
                qx[QX0 + e, t] = gx
                qy[QY0 + e, t] = gy
                acc[e] = acc[e] + (gx * gx + gy * gy)
                here = below_row
        return 0

    lax.fori_loop(0, z.bt, band_tile, 0)
    for lo, hi in runs:
        for e in range(lo, hi):
            sums[e : e + 1, :] = jnp.sum(acc[e], axis=0, keepdims=True)


def masks(z, edge):
    rows = {M - 1: edge[0:1, :], M + z.r - 1: edge[1:2, :]}
    cut = z.c - LANES
    tail = jnp.broadcast_to(edge[2:3, cut : z.ec], (8, z.ec - cut))

    def across(e, d):
        return d * rows[e] if e in rows else d

    def along(d):
        return jnp.concatenate([d[:, 0:cut], d[:, cut : z.ec] * tail], axis=1)

    return across, along


def message_rows(z, k):
    lo, hi = k, z.er - 1 - k
    return lo, hi - lo + (hi - lo) % 2


def message_shape(z, k):
    return (message_rows(z, k)[1] * (z.c // LANES) + 8, LANES)


def write_message(z, k, acc, sums, msg):
    lo, hi = k, z.er - 1 - k
    sums[...] = jnp.zeros_like(sums)
    for e in range(lo, hi):
        sums[e : e + 1, :] = jnp.sum(acc[e], axis=0, keepdims=True)
    pack_message(z, k, sums, msg)


def pack_message(z, k, sums, msg):
    first, n = message_rows(z, k)
    for t in range(z.c // LANES):
        msg[t * n : (t + 1) * n, :] = sums[first : first + n, t * LANES : (t + 1) * LANES]
    halo = [sums[8 * g : 8 * g + 8, z.c : z.ec] for g in range(z.er // 8)]
    msg[n * (z.c // LANES) :, :] = pack_lanes(halo, LANES - M, 2 * M)[0]


def read_scale(z, k, msg_a, msg_b, wx, sums, scale):
    lo, hi = k, z.er - 1 - k
    first, n = message_rows(z, k)
    lane = lane_iota((8, LANES))
    sums[...] = jnp.zeros_like(sums)
    for t in range(z.c // LANES):
        part = slice(t * n, (t + 1) * n)
        sums[first : first + n, t * LANES : (t + 1) * LANES] = msg_a[part, :] + msg_b[part, :]
    packed = msg_a[n * (z.c // LANES) :, :] + msg_b[n * (z.c // LANES) :, :]
    for g in range(z.er // 8):
        got = pltpu.roll(packed, (LANES - M - g * 2 * M) % LANES, axis=1)
        sums[8 * g : 8 * g + 8, z.c : z.ec] = jnp.where((lane < M) | (lane >= LANES - M), got, 0.0)
    w = wx[...]
    sums[...] = w / jnp.maximum(w, jnp.sqrt(1.0 + (SIGMA * SIGMA) * sums[...]))
    for e in range(lo, hi):
        scale[e] = jnp.broadcast_to(sums[e : e + 1, :], (8, z.ec))


def frame_rows(z, place, ne_in, qx_in, qy_in, wx_in, sums_in, edge, a_keep, a_send, b_keep, b_send, cor_a, cor_b, ne, qx, qy, wx, msg, acc, sums):
    core, odd = place[0], place[2]
    lane = lane_iota((8, LANES))
    sub = lax.broadcasted_iota(jnp.int32, (8, z.c), 0)
    per = LANES // (2 * M)
    q4 = z.rest

    for keep, send, first in ((a_keep, a_send, (1 - odd) * (M + z.r)), (b_keep, b_send, odd * (M + z.r))):
        for i in range(M):
            e = NE0 + first + i
            for bt in range(z.ft):
                ne[e, core * z.ft + bt, :, 0 : z.c] = keep[z.ft * i + bt]
                ne[e, (1 - core) * z.ft + bt, :, 0 : z.c] = send[z.ft * i + bt]
            k, s = keep[z.ft * M + i // 2], send[z.ft * M + i // 2]
            k0, s0 = jnp.where(core == 0, k, s), jnp.where(core == 0, s, k)
            if i % 2 == 0:
                s0 = pltpu.roll(s0, q4, axis=0)
            else:
                k0 = pltpu.roll(k0, q4, axis=0)
            ne[e, 2 * z.ft, :, 0 : z.c] = jnp.where(sub < q4, k0, s0)

    n_cor = cor_a.shape[0] - z.lt
    below = [jnp.where(odd == 0, cor_a[v], cor_b[v]) for v in range(n_cor + z.lt)]
    above = [jnp.where(odd == 0, cor_b[v], cor_a[v]) for v in range(n_cor + z.lt)]

    def corner(got, k):
        v, p = divmod(k, per)
        moved = pltpu.roll(got[v], (LANES - M - p * 2 * M) % LANES, axis=1)
        return jnp.where((lane < M) | (lane >= LANES - M), moved, 0.0)

    for r in range(M):
        for t in range(z.bt):
            ne[NE0 + M + z.r + r, t, :, z.c : z.ec] = corner(below, r * z.bt + t)
            ne[NE0 + r, t, :, z.c : z.ec] = corner(above, r * z.bt + t)
    wx[...] = wx_in[...]
    for t in range(z.lt):
        lanes = slice(t * LANES, (t + 1) * LANES)
        wx[M + z.r : z.er, lanes] = below[n_cor + t][0:M]
        wx[0:M, lanes] = above[n_cor + t][8 - M : 8]
    wx[M + z.r : z.er, z.c : z.ec] = corner(below, M * z.bt)[0:M]
    wx[0:M, z.c : z.ec] = corner(above, M * z.bt)[8 - M : 8]
    sums[...] = sums_in[...]
    first_q(z, ne, edge, [(0, M), (M + z.r - 1, z.er - 1)], qx, qy, acc, sums)
    pack_message(z, 0, sums, msg)


CARRY = 1.0 / (1.0 + TAU)
GAIN = TAU / (1.0 + TAU)


def rest_of_update(z, k, ne, u, base):
    def band_tile(t, _):
        for e in range(k + 1, z.er - 1 - k):
            base[NE0 + e, t] = CARRY * u[U0 + e, t] + GAIN * ne[NE0 + e, t]
        return 0

    lax.fori_loop(0, z.bt, band_tile, 0)


def step(z, k, base, wx, edge, u_in, qx_in, qy_in, msg_a, msg_b, u, qx, qy, msg, sums, scale, acc, ubs):
    lo, hi = k, z.er - 1 - k
    read_scale(z, k, msg_a, msg_b, wx, sums, scale)
    acc[...] = jnp.zeros_like(acc)
    across, along = masks(z, edge)

    def band_tile(t, _):
        px0 = scale[lo] * qx_in[QX0 + lo, t]
        for e in range(lo + 1, hi):
            sc = scale[e]
            px = sc * qx_in[QX0 + e, t]
            py = sc * qy_in[QY0 + e, t]
            div = ((px - px0) + py) - pltpu.roll(py, 1, axis=1)
            old = u_in[(NE0 if k == 0 else U0) + e, t]
            new = (old if k == 0 else base[NE0 + e, t]) + (GAIN * SIGMA) * div
            u[U0 + e, t] = new
            ubs[e] = (new - old) + new
            px0 = px
        ub0 = ubs[lo + 1]
        for e in range(lo + 1, hi - 1):
            sc = scale[e]
            ub = ubs[e + 1]
            nx = sc * qx_in[QX0 + e, t] + across(e, ub - ub0)
            ny = sc * qy_in[QY0 + e, t] + along(pltpu.roll(ub0, z.ec - 1, axis=1) - ub0)
            qx[QX0 + e, t] = nx
            qy[QY0 + e, t] = ny
            acc[e] = acc[e] + (nx * nx + ny * ny)
            ub0 = ub
        return 0

    lax.fori_loop(0, z.bt, band_tile, 0)
    write_message(z, k + 1, acc, sums, msg)


def last_step(z, k, own, place, base, wx, qx_in, qy_in, msg_a, msg_b, *refs):
    part = refs[0]
    sums, scale, u = refs[-3:]
    lo, hi = k, z.er - 1 - k
    core, half = place[0], place[1]
    slot = (core if own else 1 - core) * z.ft
    q4 = z.rest
    read_scale(z, k, msg_a, msg_b, wx, sums, scale)

    def band_tile(i, _):
        t = jnp.where(i == z.ft, 2 * z.ft, slot + i)
        px0 = scale[lo] * qx_in[QX0 + lo, t]
        for e in range(lo + 1, hi):
            sc = scale[e]
            px = sc * qx_in[QX0 + e, t]
            py = sc * qy_in[QY0 + e, t]
            div = ((px - px0) + py) - pltpu.roll(py, 1, axis=1)
            new = base[NE0 + e, t] + (GAIN * SIGMA) * div
            u[e - M, i] = new[:, 0 : z.c]
            px0 = px
        return 0

    lax.fori_loop(0, z.ft + 1, band_tile, 0)
    low = (core == 0) if own else (core == 1)
    for r in range(z.r):
        g, q = divmod(r, 8)
        for t in range(z.lt):
            lanes = slice(t * LANES, (t + 1) * LANES)
            run = flat_rows(part, g, t)
            for bt in range(z.ft):
                run[pl.ds(64 * bt + q, 8, stride=8), :] = u[r, bt, :, lanes]
            a, b = u[r, z.ft, 0:q4, lanes], u[r, z.ft, q4:8, lanes]
            run[pl.ds(8 * z.full + q, q4, stride=8), :] = jnp.where(low, a, b)


def write_out(z, place, keep, recv, out, sem_k, sem_r):
    half = place[1]
    copies = half_copies(z, half, out, keep, sem_k, out=True) + half_copies(z, 1 - half, out, recv, sem_r, out=True)
    for c in copies:
        c.start()
    for c in copies:
        c.wait()


def local(noisy, weight_map):
    z = Sizes(*noisy.shape)
    n_row, n_col, n_band = (lax.axis_size(a) for a in ("row", "col", "band"))
    chips = n_band // 2
    core = lax.axis_index("band") % 2
    half = core ^ (lax.axis_index("band") // 2 % 2)
    row0 = lax.axis_index("row") * z.r
    col0 = lax.axis_index("col") * (2 * z.c) + half * z.c

    lane = jnp.arange(z.ec)
    gcol = col0 + jnp.where(lane < z.c + LANES // 2, lane, lane - z.ec)
    inner = (gcol >= 0) & (gcol < n_col * 2 * z.c - 1)
    edge = jnp.stack([
        jnp.broadcast_to(row0 > 0, (z.ec,)), jnp.broadcast_to(row0 + z.r < n_row * z.r, (z.ec,)), inner,
    ] + [inner] * 5).astype(F32)

    def at(chip, h):
        return 2 * chip + (h ^ (chip % 2))

    swap = [(i, i ^ 1) for i in range(n_band)]
    pair_a = [(at(c, h), at(c ^ 1, h)) for c in range(chips) for h in range(2)]
    pair_b = [(at(c, h), at((c - 1 + 2 * (c % 2)) % chips, h)) for c in range(chips) for h in range(2)]
    rows_a = [(i, i ^ 1) for i in range(n_row)]
    rows_b = [(i, min(max(i - 1 + 2 * (i % 2), 0), n_row - 1)) for i in range(n_row)]
    across_a = [(i * n_band + b, j * n_band + (b ^ 1)) for i, j in rows_a for b in range(n_band)]
    across_b = [(i * n_band + b, j * n_band + (b ^ 1)) for i, j in rows_b for b in range(n_band)]
    spot = [[(j // 2) * n_band + at(c, j % 2) for j in range(2 * n_col)] for c in range(chips)]
    to_right = [(line[j], line[(j + 1) % len(line)]) for line in spot for j in range(len(line))]
    to_left = [(b, a) for a, b in to_right]

    odd = lax.axis_index("row") % 2
    place = jnp.stack([core, half, odd]).astype(jnp.int32)
    place, edge = lax.optimization_barrier((place, edge))
    w = weight_map

    units = z.r * z.bt + z.r // 8
    n_edge = -(-units // (LANES // M))
    n_corner = -(-(M * z.bt + 1) // (LANES // (2 * M)))
    state = (z.er + 4, z.bt, 8, z.ec)
    flat = (z.er, z.ec)
    side = (n_edge, 8, LANES)
    bulk = (z.ft * M + M * z.rest // 8, 8, z.c)
    corner = (n_corner + z.lt, 8, LANES)
    cost = z.er * z.nb * z.ec
    sem = pltpu.SemaphoreType.DMA((z.rg * z.lt,))

    keep, send, a_keep, a_send, b_keep, b_send = call(
        lambda *a: split(z, *a), [z.block, z.block] + [bulk] * 4,
        [place, pltpu.with_memory_space_constraint(noisy, pltpu.HBM)],
        n_smem=1, scratch=[sem, sem], hbm_in=(1,), flops=cost,
    )
    far = [
        lax.ppermute(a_keep, "row", rows_a), lax.ppermute(a_send, ("row", "band"), across_a),
        lax.ppermute(b_keep, "row", rows_b), lax.ppermute(b_send, ("row", "band"), across_b),
    ]
    recv = lax.ppermute(send, "band", swap)
    ne, col_l, col_r = call(
        lambda *a: assemble(z, *a), [state, side, side], [place, keep, recv, w, edge], n_smem=1, flops=cost
    )
    from_r = lax.ppermute(col_l, ("col", "band"), to_left)
    from_l = lax.ppermute(col_r, ("col", "band"), to_right)
    acc = pltpu.VMEM((z.er, 8, z.ec), F32)
    one = pltpu.VMEM(flat, F32)
    ne, wx, qx, qy, sums, cor_a, cor_b = call(
        lambda *a: frame_cols(z, *a), [state, flat, state, state, flat, corner, corner],
        [place, ne, w, edge, from_r, from_l], n_smem=1, aliases={1: 0}, scratch=[acc], flops=5 * cost,
    )
    cor_a = lax.ppermute(cor_a, "row", rows_a)
    cor_b = lax.ppermute(cor_b, "row", rows_b)
    ne, qx, qy, wx, msg = call(
        lambda *a: frame_rows(z, *a), [state, state, state, flat, message_shape(z, 0)],
        [place, ne, qx, qy, wx, sums, edge, *far, cor_a, cor_b],
        n_smem=1, aliases={1: 0, 2: 1, 3: 2}, scratch=[acc, one], flops=5 * cost,
    )
    u = base = ne
    for k in range(ITERS):
        msg = msg + lax.ppermute(msg, "band", pair_a)
        other = lax.ppermute(msg, "band", pair_b)
        if k > 0:
            (base,) = call(lambda *a, k=k: rest_of_update(z, k, *a), [state], [ne, u], flops=cost)
        if k < ITERS - 1:
            u, qx, qy, msg = call(
                lambda *a, k=k: step(z, k, *a), [state, state, state, message_shape(z, k + 1)],
                [base, wx, edge, u, qx, qy, msg, other], scratch=[one, acc, acc, acc], flops=20 * cost,
            )
    last = [place, base, wx, qx, qy, msg, other]
    room = [one, acc, pltpu.VMEM((z.r, z.ft + 1, 8, z.c), F32)]
    (send,) = call(lambda *a: last_step(z, ITERS - 1, False, *a), [z.block], last, n_smem=1, scratch=room, flops=5 * cost)
    recv = lax.ppermute(send, "band", swap)
    (keep,) = call(lambda *a: last_step(z, ITERS - 1, True, *a), [z.block], last, n_smem=1, scratch=room, flops=5 * cost)
    (out,) = call(
        lambda *a: write_out(z, *a), [noisy.shape], [place, keep, recv],
        n_smem=1, scratch=[sem, sem], hbm_out=(0,), flops=cost,
    )
    return out


def solution(mesh):
    placed = (P("band", "row", "col"), P("row", "col"))
    return jax.shard_map(
        local, mesh=mesh, in_specs=placed, out_specs=P("band", "row", "col"), check_vma=False
    )
```

```python
import jax
import jax.numpy as jnp
from jax import lax
from jax.experimental import pallas as pl
from jax.experimental.pallas import tpu as pltpu
from jax.sharding import PartitionSpec as P

ITERS = 4
M = ITERS
LANES = 128
SIGMA = 0.35
TAU = 0.35


F32 = jnp.float32
U0, QX0, QY0, NE0 = range(4)
VM = pl.BlockSpec(memory_space=pltpu.VMEM)
SM = pl.BlockSpec(memory_space=pltpu.SMEM)
HB = pl.BlockSpec(memory_space=pltpu.HBM)
PARAMS = pltpu.CompilerParams(vmem_limit_bytes=8 * 1024 * 1024)


def call(body, outs, ins, n_smem=0, aliases=None, scratch=(), flops=0, hbm_in=(), hbm_out=()):
    in_specs = [SM] * n_smem + [VM] * (len(ins) - n_smem)
    return pl.pallas_call(
        body,
        out_shape=[(pltpu.HBM if i in hbm_out else pltpu.VMEM)(s, F32) for i, s in enumerate(outs)],
        in_specs=[HB if i in hbm_in else spec for i, spec in enumerate(in_specs)],
        out_specs=[HB if i in hbm_out else VM for i in range(len(outs))],
        scratch_shapes=list(scratch),
        input_output_aliases=aliases or {},
        compiler_params=PARAMS,
        cost_estimate=pl.CostEstimate(flops=flops, bytes_accessed=0, transcendentals=0),
    )(*ins)


def here():
    band = lax.axis_index("band")
    core = lax.rem(band, 2)
    return core, core ^ lax.rem(lax.div(band, 2), 2), lax.rem(lax.axis_index("row"), 2)


def lane_iota(shape):
    return lax.broadcasted_iota(jnp.int32, shape, len(shape) - 1)


class Sizes:
    def __init__(self, bands, rows, cols):
        self.b = bands
        self.nb = 2 * bands
        self.bt = self.nb // 8
        self.r = rows
        self.c = cols // 2
        self.er = rows + 2 * M
        self.ec = self.c + LANES
        self.full = self.b // 8 * 8
        self.rest = self.b - self.full
        self.ft = self.full // 8
        self.rg = rows // 8
        self.lt = self.c // LANES
        self.block = (self.rg, self.lt, self.b, 8, LANES)


def pack_lanes(tiles, first, width):
    per = LANES // width
    lane = lane_iota((8, LANES))
    out = []
    for v in range(0, len(tiles), per):
        acc = None
        for p, tile in enumerate(tiles[v : v + per]):
            moved = pltpu.roll(tile, (p * width - first) % LANES, axis=1)
            acc = moved if acc is None else jnp.where(lane // width == p, moved, acc)
        out.append(acc)
    return out


def flat_rows(ref, *at):
    tile = ref.at[at]
    return tile.reshape(tile.shape[0] * 8, LANES)


def half_copies(z, half, array, block, sem, out=False):
    copies = []
    for g in range(z.rg):
        for t in range(z.lt):
            lanes = pl.ds(pl.multiple_of(half * z.c + t * LANES, LANES), LANES)
            ends = [array.at[:, pl.ds(8 * g, 8), lanes], block.at[g, t]]
            copies.append(pltpu.make_async_copy(*(ends[::-1] if out else ends), sem.at[g * z.lt + t]))
    return copies


def split(z, place, noisy, keep, send, a_keep, a_send, b_keep, b_send, sem_k, sem_s):
    half, odd = place[1], place[2]
    kept, sent = half_copies(z, half, noisy, keep, sem_k), half_copies(z, 1 - half, noisy, send, sem_s)
    groups = [kept[g * z.lt : (g + 1) * z.lt] + sent[g * z.lt : (g + 1) * z.lt] for g in range(z.rg)]
    for c in sum(groups, []):
        c.start()

    def rows(block, first, msg):
        for i in range(M):
            g, q = divmod(first + i, 8)
            for t in range(z.lt):
                run = flat_rows(block, g, t)
                lanes = slice(t * LANES, (t + 1) * LANES)
                for bt in range(z.ft):
                    msg[z.ft * i + bt, :, lanes] = run[pl.ds(64 * bt + q, 8, stride=8), :]
                at = z.rest * (i % 2)
                msg[z.ft * M + i // 2, at : at + z.rest, lanes] = run[pl.ds(8 * z.full + q, z.rest, stride=8), :]

    def gather(first, even, other):
        @pl.when(odd == 0)
        def _():
            rows(keep, first, even[0])
            rows(send, first, even[1])

        @pl.when(odd == 1)
        def _():
            rows(keep, first, other[0])
            rows(send, first, other[1])

    for n, copies in enumerate(groups):
        for c in copies:
            c.wait()
        if n == 0:
            gather(0, (b_keep, b_send), (a_keep, a_send))
        if n == z.rg - 1:
            gather(z.r - M, (a_keep, a_send), (b_keep, b_send))


def half_of(z, place, w):
    return jnp.where(place[1] == 0, w[:, 0 : z.c], w[:, z.c : 2 * z.c])


def assemble(z, place, keep, recv, w_whole, edge, ne, col_l, col_r):
    core = place[0]
    w = half_of(z, place, w_whole)
    q4 = z.rest
    for r in range(z.r):
        g, q = divmod(r, 8)
        for t in range(z.lt):
            lanes = slice(t * LANES, (t + 1) * LANES)
            mine, other = flat_rows(keep, g, t), flat_rows(recv, g, t)
            for bt in range(z.ft):
                ne[NE0 + M + r, core * z.ft + bt, :, lanes] = mine[pl.ds(64 * bt + q, 8, stride=8), :]
                ne[NE0 + M + r, (1 - core) * z.ft + bt, :, lanes] = other[pl.ds(64 * bt + q, 8, stride=8), :]
            a = mine[pl.ds(8 * z.full + q, q4, stride=8), :]
            b = other[pl.ds(8 * z.full + q, q4, stride=8), :]
            ne[NE0 + M + r, 2 * z.ft, 0:q4, lanes] = jnp.where(core == 0, a, b)
            ne[NE0 + M + r, 2 * z.ft, q4:8, lanes] = jnp.where(core == 0, b, a)
    last = slice(z.c - LANES, z.c)
    left = [ne[NE0 + M + r, t, :, 0:LANES] for r in range(z.r) for t in range(z.bt)]
    left += [w[8 * t : 8 * t + 8, 0:LANES] for t in range(z.r // 8)]
    right = [ne[NE0 + M + r, t, :, last] for r in range(z.r) for t in range(z.bt)]
    right += [w[8 * t : 8 * t + 8, last] for t in range(z.r // 8)]
    for v, tile in enumerate(pack_lanes(left, 0, M)):
        col_l[v] = tile
    for v, tile in enumerate(pack_lanes(right, LANES - M, M)):
        col_r[v] = tile


def frame_cols(z, place, ne_in, w_whole, edge, from_r, from_l, ne, wx, qx, qy, sums, cor_a, cor_b, acc):
    w = half_of(z, place, w_whole)
    lane = lane_iota((8, LANES))
    per = LANES // M
    units = z.r * z.bt + z.r // 8
    tiles = []
    for k in range(units):
        v, p = divmod(k, per)
        hi = pltpu.roll(from_r[v], (-p * M) % LANES, axis=1)
        lo = pltpu.roll(from_l[v], (LANES - M - p * M) % LANES, axis=1)
        tiles.append(jnp.where(lane < M, hi, jnp.where(lane >= LANES - M, lo, 0.0)))
    for r in range(z.r):
        for t in range(z.bt):
            ne[NE0 + M + r, t, :, z.c : z.ec] = tiles[r * z.bt + t]
    wx[0:M, :] = jnp.zeros((M, z.ec), F32)
    wx[M + z.r : z.er, :] = jnp.zeros((M, z.ec), F32)
    wx[M : M + z.r, 0 : z.c] = w
    for t in range(z.r // 8):
        wx[M + 8 * t : M + 8 * t + 8, z.c : z.ec] = tiles[z.r * z.bt + t]
    up = tiles[: M * z.bt] + [tiles[z.r * z.bt]]
    down = tiles[(z.r - M) * z.bt : z.r * z.bt] + [tiles[units - 1]]
    up, down = (pack_lanes(x, LANES - M, 2 * M) for x in (up, down))
    lanes = [slice(t * LANES, (t + 1) * LANES) for t in range(z.lt)]
    up += [w[0:8, x] for x in lanes]
    down += [w[z.r - 8 : z.r, x] for x in lanes]
    odd = place[2]
    for v, (u, d) in enumerate(zip(up, down)):
        cor_a[v] = jnp.where(odd == 0, d, u)
        cor_b[v] = jnp.where(odd == 0, u, d)
    sums[...] = jnp.zeros_like(sums)
    first_q(z, ne, edge, [(M, M + z.r - 1)], qx, qy, acc, sums)


def first_q(z, ne, edge, runs, qx, qy, acc, sums):
    across, along = masks(z, edge)
    acc[...] = jnp.zeros_like(acc)

    def band_tile(t, _):
        for lo, hi in runs:
            here = ne[NE0 + lo, t]
            for e in range(lo, hi):
                below_row = ne[NE0 + e + 1, t]
                gx = across(e, below_row - here)
                gy = along(pltpu.roll(here, z.ec - 1, axis=1) - here)
                qx[QX0 + e, t] = gx
                qy[QY0 + e, t] = gy
                acc[e] = acc[e] + (gx * gx + gy * gy)
                here = below_row
        return 0

    lax.fori_loop(0, z.bt, band_tile, 0)
    for lo, hi in runs:
        for e in range(lo, hi):
            sums[e : e + 1, :] = jnp.sum(acc[e], axis=0, keepdims=True)


def masks(z, edge):
    rows = {M - 1: edge[0:1, :], M + z.r - 1: edge[1:2, :]}
    cut = z.c - LANES
    tail = jnp.broadcast_to(edge[2:3, cut : z.ec], (8, z.ec - cut))

    def across(e, d):
        return d * rows[e] if e in rows else d

    def along(d):
        return jnp.concatenate([d[:, 0:cut], d[:, cut : z.ec] * tail], axis=1)

    return across, along


def message_rows(z, k):
    lo, hi = k, z.er - 1 - k
    return lo, hi - lo + (hi - lo) % 2


def message_shape(z, k):
    return (message_rows(z, k)[1] * (z.c // LANES) + 8, LANES)


def write_message(z, k, acc, sums, msg):
    lo, hi = k, z.er - 1 - k
    sums[...] = jnp.zeros_like(sums)
    for e in range(lo, hi):
        sums[e : e + 1, :] = jnp.sum(acc[e], axis=0, keepdims=True)
    pack_message(z, k, sums, msg)


def pack_message(z, k, sums, msg):
    first, n = message_rows(z, k)
    for t in range(z.c // LANES):
        msg[t * n : (t + 1) * n, :] = sums[first : first + n, t * LANES : (t + 1) * LANES]
    halo = [sums[8 * g : 8 * g + 8, z.c : z.ec] for g in range(z.er // 8)]
    msg[n * (z.c // LANES) :, :] = pack_lanes(halo, LANES - M, 2 * M)[0]


def read_scale(z, k, msg_a, msg_b, wx, sums, scale):
    lo, hi = k, z.er - 1 - k
    first, n = message_rows(z, k)
    lane = lane_iota((8, LANES))
    sums[...] = jnp.zeros_like(sums)
    for t in range(z.c // LANES):
        part = slice(t * n, (t + 1) * n)
        sums[first : first + n, t * LANES : (t + 1) * LANES] = msg_a[part, :] + msg_b[part, :]
    packed = msg_a[n * (z.c // LANES) :, :] + msg_b[n * (z.c // LANES) :, :]
    for g in range(z.er // 8):
        got = pltpu.roll(packed, (LANES - M - g * 2 * M) % LANES, axis=1)
        sums[8 * g : 8 * g + 8, z.c : z.ec] = jnp.where((lane < M) | (lane >= LANES - M), got, 0.0)
    w = wx[...]
    sums[...] = w / jnp.maximum(w, jnp.sqrt(1.0 + (SIGMA * SIGMA) * sums[...]))
    for e in range(lo, hi):
        scale[e] = jnp.broadcast_to(sums[e : e + 1, :], (8, z.ec))


def frame_rows(z, place, ne_in, qx_in, qy_in, wx_in, sums_in, edge, a_keep, a_send, b_keep, b_send, cor_a, cor_b, ne, qx, qy, wx, msg, acc, sums):
    core, odd = place[0], place[2]
    lane = lane_iota((8, LANES))
    sub = lax.broadcasted_iota(jnp.int32, (8, z.c), 0)
    per = LANES // (2 * M)
    q4 = z.rest

    for keep, send, first in ((a_keep, a_send, (1 - odd) * (M + z.r)), (b_keep, b_send, odd * (M + z.r))):
        for i in range(M):
            e = NE0 + first + i
            for bt in range(z.ft):
                ne[e, core * z.ft + bt, :, 0 : z.c] = keep[z.ft * i + bt]
                ne[e, (1 - core) * z.ft + bt, :, 0 : z.c] = send[z.ft * i + bt]
            k, s = keep[z.ft * M + i // 2], send[z.ft * M + i // 2]
            k0, s0 = jnp.where(core == 0, k, s), jnp.where(core == 0, s, k)
            if i % 2 == 0:
                s0 = pltpu.roll(s0, q4, axis=0)
            else:
                k0 = pltpu.roll(k0, q4, axis=0)
            ne[e, 2 * z.ft, :, 0 : z.c] = jnp.where(sub < q4, k0, s0)

    n_cor = cor_a.shape[0] - z.lt
    below = [jnp.where(odd == 0, cor_a[v], cor_b[v]) for v in range(n_cor + z.lt)]
    above = [jnp.where(odd == 0, cor_b[v], cor_a[v]) for v in range(n_cor + z.lt)]

    def corner(got, k):
        v, p = divmod(k, per)
        moved = pltpu.roll(got[v], (LANES - M - p * 2 * M) % LANES, axis=1)
        return jnp.where((lane < M) | (lane >= LANES - M), moved, 0.0)

    for r in range(M):
        for t in range(z.bt):
            ne[NE0 + M + z.r + r, t, :, z.c : z.ec] = corner(below, r * z.bt + t)
            ne[NE0 + r, t, :, z.c : z.ec] = corner(above, r * z.bt + t)
    wx[...] = wx_in[...]
    for t in range(z.lt):
        lanes = slice(t * LANES, (t + 1) * LANES)
        wx[M + z.r : z.er, lanes] = below[n_cor + t][0:M]
        wx[0:M, lanes] = above[n_cor + t][8 - M : 8]
    wx[M + z.r : z.er, z.c : z.ec] = corner(below, M * z.bt)[0:M]
    wx[0:M, z.c : z.ec] = corner(above, M * z.bt)[8 - M : 8]
    sums[...] = sums_in[...]
    first_q(z, ne, edge, [(0, M), (M + z.r - 1, z.er - 1)], qx, qy, acc, sums)
    pack_message(z, 0, sums, msg)


CARRY = 1.0 / (1.0 + TAU)
GAIN = TAU / (1.0 + TAU)


def rest_of_update(z, k, ne, u, base):
    def band_tile(t, _):
        for e in range(k + 1, z.er - 1 - k):
            base[NE0 + e, t] = CARRY * u[U0 + e, t] + GAIN * ne[NE0 + e, t]
        return 0

    lax.fori_loop(0, z.bt, band_tile, 0)


def step(z, k, base, wx, edge, u_in, qx_in, qy_in, msg_a, msg_b, u, qx, qy, msg, sums, scale, acc, ubs, pxs, pys):
    lo, hi = k, z.er - 1 - k
    read_scale(z, k, msg_a, msg_b, wx, sums, scale)
    acc[...] = jnp.zeros_like(acc)
    across, along = masks(z, edge)

    def band_tile(t, _):
        px0 = scale[lo] * qx_in[QX0 + lo, t]
        for e in range(lo + 1, hi):
            sc = scale[e]
            px = sc * qx_in[QX0 + e, t]
            py = sc * qy_in[QY0 + e, t]
            div = ((px - px0) + py) - pltpu.roll(py, 1, axis=1)
            old = u_in[(NE0 if k == 0 else U0) + e, t]
            new = (old if k == 0 else base[NE0 + e, t]) + (GAIN * SIGMA) * div
            u[U0 + e, t] = new
            ubs[e] = (new - old) + new
            pxs[e], pys[e] = px, py
            px0 = px
        ub0 = ubs[lo + 1]
        for e in range(lo + 1, hi - 1):
            ub = ubs[e + 1]
            nx = pxs[e] + across(e, ub - ub0)
            ny = pys[e] + along(pltpu.roll(ub0, z.ec - 1, axis=1) - ub0)
            qx[QX0 + e, t] = nx
            qy[QY0 + e, t] = ny
            acc[e] = acc[e] + (nx * nx + ny * ny)
            ub0 = ub
        return 0

    lax.fori_loop(0, z.bt, band_tile, 0)
    write_message(z, k + 1, acc, sums, msg)


def last_step(z, k, own, place, base, wx, qx_in, qy_in, msg_a, msg_b, *refs):
    part = refs[0]
    sums, scale, u = refs[-3:]
    lo, hi = k, z.er - 1 - k
    core, half = place[0], place[1]
    slot = (core if own else 1 - core) * z.ft
    q4 = z.rest
    read_scale(z, k, msg_a, msg_b, wx, sums, scale)

    def band_tile(i, _):
        t = jnp.where(i == z.ft, 2 * z.ft, slot + i)
        px0 = scale[lo] * qx_in[QX0 + lo, t]
        for e in range(lo + 1, hi):
            sc = scale[e]
            px = sc * qx_in[QX0 + e, t]
            py = sc * qy_in[QY0 + e, t]
            div = ((px - px0) + py) - pltpu.roll(py, 1, axis=1)
            new = base[NE0 + e, t] + (GAIN * SIGMA) * div
            u[e - M, i] = new[:, 0 : z.c]
            px0 = px
        return 0

    lax.fori_loop(0, z.ft + 1, band_tile, 0)
    low = (core == 0) if own else (core == 1)
    for r in range(z.r):
        g, q = divmod(r, 8)
        for t in range(z.lt):
            lanes = slice(t * LANES, (t + 1) * LANES)
            run = flat_rows(part, g, t)
            for bt in range(z.ft):
                run[pl.ds(64 * bt + q, 8, stride=8), :] = u[r, bt, :, lanes]
            a, b = u[r, z.ft, 0:q4, lanes], u[r, z.ft, q4:8, lanes]
            run[pl.ds(8 * z.full + q, q4, stride=8), :] = jnp.where(low, a, b)


def write_out(z, place, keep, recv, out, sem_k, sem_r):
    half = place[1]
    copies = half_copies(z, half, out, keep, sem_k, out=True) + half_copies(z, 1 - half, out, recv, sem_r, out=True)
    for c in copies:
        c.start()
    for c in copies:
        c.wait()


def local(noisy, weight_map):
    z = Sizes(*noisy.shape)
    n_row, n_col, n_band = (lax.axis_size(a) for a in ("row", "col", "band"))
    chips = n_band // 2
    _, half, _ = here()
    row0 = lax.axis_index("row") * z.r
    col0 = lax.axis_index("col") * (2 * z.c) + half * z.c

    lane = jnp.arange(z.ec)
    gcol = col0 + jnp.where(lane < z.c + LANES // 2, lane, lane - z.ec)
    inner = (gcol >= 0) & (gcol < n_col * 2 * z.c - 1)
    edge = jnp.stack([
        jnp.broadcast_to(row0 > 0, (z.ec,)), jnp.broadcast_to(row0 + z.r < n_row * z.r, (z.ec,)), inner,
    ] + [inner] * 5).astype(F32)

    def at(chip, h):
        return 2 * chip + (h ^ (chip % 2))

    swap = [(i, i ^ 1) for i in range(n_band)]
    pair_a = [(at(c, h), at(c ^ 1, h)) for c in range(chips) for h in range(2)]
    pair_b = [(at(c, h), at((c - 1 + 2 * (c % 2)) % chips, h)) for c in range(chips) for h in range(2)]
    rows_a = [(i, i ^ 1) for i in range(n_row)]
    rows_b = [(i, min(max(i - 1 + 2 * (i % 2), 0), n_row - 1)) for i in range(n_row)]
    across_a = [(i * n_band + b, j * n_band + (b ^ 1)) for i, j in rows_a for b in range(n_band)]
    across_b = [(i * n_band + b, j * n_band + (b ^ 1)) for i, j in rows_b for b in range(n_band)]
    spot = [[(j // 2) * n_band + at(c, j % 2) for j in range(2 * n_col)] for c in range(chips)]
    to_right = [(line[j], line[(j + 1) % len(line)]) for line in spot for j in range(len(line))]
    to_left = [(b, a) for a, b in to_right]

    (edge,) = lax.optimization_barrier((edge,))
    w = weight_map

    units = z.r * z.bt + z.r // 8
    n_edge = -(-units // (LANES // M))
    n_corner = -(-(M * z.bt + 1) // (LANES // (2 * M)))
    state = (z.er + 4, z.bt, 8, z.ec)
    flat = (z.er, z.ec)
    side = (n_edge, 8, LANES)
    bulk = (z.ft * M + M * z.rest // 8, 8, z.c)
    corner = (n_corner + z.lt, 8, LANES)
    cost = z.er * z.nb * z.ec
    sem = pltpu.SemaphoreType.DMA((z.rg * z.lt,))

    keep, send, a_keep, a_send, b_keep, b_send = call(
        lambda *a: split(z, here(), *a), [z.block, z.block] + [bulk] * 4,
        [pltpu.with_memory_space_constraint(noisy, pltpu.HBM)],
        scratch=[sem, sem], hbm_in=(0,), flops=cost,
    )
    far = [
        lax.ppermute(a_keep, "row", rows_a), lax.ppermute(a_send, ("row", "band"), across_a),
        lax.ppermute(b_keep, "row", rows_b), lax.ppermute(b_send, ("row", "band"), across_b),
    ]
    recv = lax.ppermute(send, "band", swap)
    ne, col_l, col_r = call(
        lambda *a: assemble(z, here(), *a), [state, side, side], [keep, recv, w, edge], flops=cost
    )
    from_r = lax.ppermute(col_l, ("col", "band"), to_left)
    from_l = lax.ppermute(col_r, ("col", "band"), to_right)
    acc = pltpu.VMEM((z.er, 8, z.ec), F32)
    one = pltpu.VMEM(flat, F32)
    ne, wx, qx, qy, sums, cor_a, cor_b = call(
        lambda *a: frame_cols(z, here(), *a), [state, flat, state, state, flat, corner, corner],
        [ne, w, edge, from_r, from_l], aliases={0: 0}, scratch=[acc], flops=5 * cost,
    )
    cor_a = lax.ppermute(cor_a, "row", rows_a)
    cor_b = lax.ppermute(cor_b, "row", rows_b)
    ne, qx, qy, wx, msg = call(
        lambda *a: frame_rows(z, here(), *a), [state, state, state, flat, message_shape(z, 0)],
        [ne, qx, qy, wx, sums, edge, *far, cor_a, cor_b],
        aliases={0: 0, 1: 1, 2: 2}, scratch=[acc, one], flops=5 * cost,
    )
    u = base = ne
    for k in range(ITERS):
        msg = msg + lax.ppermute(msg, "band", pair_a)
        other = lax.ppermute(msg, "band", pair_b)
        if k > 0:
            (base,) = call(lambda *a, k=k: rest_of_update(z, k, *a), [state], [ne, u], flops=cost)
        if k < ITERS - 1:
            u, qx, qy, msg = call(
                lambda *a, k=k: step(z, k, *a), [state, state, state, message_shape(z, k + 1)],
                [base, wx, edge, u, qx, qy, msg, other], scratch=[one, acc, acc, acc, acc, acc], flops=20 * cost,
            )
    last = [base, wx, qx, qy, msg, other]
    room = [one, acc, pltpu.VMEM((z.r, z.ft + 1, 8, z.c), F32)]
    (send,) = call(lambda *a: last_step(z, ITERS - 1, False, here(), *a), [z.block], last, scratch=room, flops=5 * cost)
    recv = lax.ppermute(send, "band", swap)
    (keep,) = call(lambda *a: last_step(z, ITERS - 1, True, here(), *a), [z.block], last, scratch=room, flops=5 * cost)
    (out,) = call(
        lambda *a: write_out(z, here(), *a), [noisy.shape], [keep, recv],
        scratch=[sem, sem], hbm_out=(0,), flops=cost,
    )
    return out


def solution(mesh):
    placed = (P("band", "row", "col"), P("row", "col"))
    return jax.shard_map(
        local, mesh=mesh, in_specs=placed, out_specs=P("band", "row", "col"), check_vma=False
    )
```

```python
import jax
import jax.numpy as jnp
from jax import lax
from jax.experimental import pallas as pl
from jax.experimental.pallas import tpu as pltpu
from jax.sharding import PartitionSpec as P


ITERS = 4
M = ITERS
LANES = 128
SIGMA = 0.35
TAU = 0.35


F32 = jnp.float32
U0, QX0, QY0, NE0 = range(4)
VM = pl.BlockSpec(memory_space=pltpu.VMEM)
SM = pl.BlockSpec(memory_space=pltpu.SMEM)
HB = pl.BlockSpec(memory_space=pltpu.HBM)
PARAMS = pltpu.CompilerParams(vmem_limit_bytes=8 * 1024 * 1024)


def call(body, outs, ins, n_smem=0, aliases=None, scratch=(), flops=0, hbm_in=(), hbm_out=()):
    in_specs = [SM] * n_smem + [VM] * (len(ins) - n_smem)
    return pl.pallas_call(
        body,
        out_shape=[(pltpu.HBM if i in hbm_out else pltpu.VMEM)(s, F32) for i, s in enumerate(outs)],
        in_specs=[HB if i in hbm_in else spec for i, spec in enumerate(in_specs)],
        out_specs=[HB if i in hbm_out else VM for i in range(len(outs))],
        scratch_shapes=list(scratch),
        input_output_aliases=aliases or {},
        compiler_params=PARAMS,
        cost_estimate=pl.CostEstimate(flops=flops, bytes_accessed=0, transcendentals=0),
    )(*ins)


def here():
    band = lax.axis_index("band")
    core = lax.rem(band, 2)
    return core, core ^ lax.rem(lax.div(band, 2), 2), lax.rem(lax.axis_index("row"), 2)


def lane_iota(shape):
    return lax.broadcasted_iota(jnp.int32, shape, len(shape) - 1)


class Sizes:
    def __init__(self, bands, rows, cols):
        self.b = bands
        self.nb = 2 * bands
        self.bt = self.nb // 8
        self.r = rows
        self.c = cols // 2
        self.er = rows + 2 * M
        self.ec = self.c + LANES
        self.full = self.b // 8 * 8
        self.rest = self.b - self.full
        self.ft = self.full // 8
        self.rg = rows // 8
        self.lt = self.c // LANES
        self.block = (self.rg, self.lt, self.b, 8, LANES)


def pack_lanes(tiles, first, width):
    per = LANES // width
    lane = lane_iota((8, LANES))
    out = []
    for v in range(0, len(tiles), per):
        acc = None
        for p, tile in enumerate(tiles[v : v + per]):
            moved = pltpu.roll(tile, (p * width - first) % LANES, axis=1)
            acc = moved if acc is None else jnp.where(lane // width == p, moved, acc)
        out.append(acc)
    return out


def flat_rows(ref, *at):
    tile = ref.at[at]
    return tile.reshape(tile.shape[0] * 8, LANES)


def half_copies(z, half, array, block, sem, group=None, out=False):
    copies = []
    for g in range(z.rg) if group is None else (None,):
        rows = pl.ds(8 * g, 8) if group is None else pl.ds(pl.multiple_of(group * 8, 8), 8)
        for t in range(z.lt):
            lanes = pl.ds(pl.multiple_of(half * z.c + t * LANES, LANES), LANES)
            ends = [array.at[:, rows, lanes], block.at[t] if group is not None else block.at[g, t]]
            copies.append(pltpu.make_async_copy(*(ends[::-1] if out else ends), sem.at[(g or 0) * z.lt + t]))
    return copies


def split(z, facing_b, place, noisy, edge, *refs):
    weights, (keep, send, msg_keep, msg_send), more = refs[0], refs[facing_b : facing_b + 4], refs[facing_b + 4 :]
    sem_k, sem_s = more[facing_b : facing_b + 2]
    half, odd = place[1], place[2]
    group = odd if facing_b else 1 - odd
    copies = half_copies(z, half, noisy, keep, sem_k, group) + half_copies(z, 1 - half, noisy, send, sem_s, group)
    if facing_b:
        lanes = pl.ds(pl.multiple_of(half * z.c, LANES), z.c)
        copies.append(pltpu.make_async_copy(weights.at[:, lanes], more[0], more[3]))
    for c in copies:
        c.start()
    for c in copies:
        c.wait()

    def rows(block, first, msg):
        for i in range(M):
            q = first + i
            for t in range(z.lt):
                run = flat_rows(block, t)
                lanes = slice(t * LANES, (t + 1) * LANES)
                for bt in range(z.ft):
                    msg[z.ft * i + bt, :, lanes] = run[pl.ds(64 * bt + q, 8, stride=8), :]
                at = z.rest * (i % 2)
                msg[z.ft * M + i // 2, at : at + z.rest, lanes] = run[pl.ds(8 * z.full + q, z.rest, stride=8), :]

    @pl.when(group == 0)
    def _():
        rows(keep, 0, msg_keep)
        rows(send, 0, msg_send)

    @pl.when(group == 1)
    def _():
        rows(keep, 8 - M, msg_keep)
        rows(send, 8 - M, msg_send)


def assemble(z, place, keep_a, send_a, keep_b, send_b, w, edge, ne, col_l, col_r):
    core, odd = place[0], place[2]
    q4 = z.rest
    for keep, recv, group in ((keep_a, send_a, 1 - odd), (keep_b, send_b, odd)):
        for q in range(8):
            e = NE0 + M + 8 * group + q
            for t in range(z.lt):
                lanes = slice(t * LANES, (t + 1) * LANES)
                mine, other = flat_rows(keep, t), flat_rows(recv, t)
                for bt in range(z.ft):
                    ne[e, core * z.ft + bt, :, lanes] = mine[pl.ds(64 * bt + q, 8, stride=8), :]
                    ne[e, (1 - core) * z.ft + bt, :, lanes] = other[pl.ds(64 * bt + q, 8, stride=8), :]
                a = mine[pl.ds(8 * z.full + q, q4, stride=8), :]
                b = other[pl.ds(8 * z.full + q, q4, stride=8), :]
                ne[e, 2 * z.ft, 0:q4, lanes] = jnp.where(core == 0, a, b)
                ne[e, 2 * z.ft, q4:8, lanes] = jnp.where(core == 0, b, a)
    last = slice(z.c - LANES, z.c)
    left = [ne[NE0 + M + r, t, :, 0:LANES] for r in range(z.r) for t in range(z.bt)]
    left += [w[8 * t : 8 * t + 8, 0:LANES] for t in range(z.r // 8)]
    right = [ne[NE0 + M + r, t, :, last] for r in range(z.r) for t in range(z.bt)]
    right += [w[8 * t : 8 * t + 8, last] for t in range(z.r // 8)]
    for v, tile in enumerate(pack_lanes(left, 0, M)):
        col_l[v] = tile
    for v, tile in enumerate(pack_lanes(right, LANES - M, M)):
        col_r[v] = tile


def frame_cols(z, place, ne_in, w, edge, from_r, from_l, ne, wx, qx, qy, sums, cor_a, cor_b, acc):
    lane = lane_iota((8, LANES))
    per = LANES // M
    units = z.r * z.bt + z.r // 8
    tiles = []
    for k in range(units):
        v, p = divmod(k, per)
        hi = pltpu.roll(from_r[v], (-p * M) % LANES, axis=1)
        lo = pltpu.roll(from_l[v], (LANES - M - p * M) % LANES, axis=1)
        tiles.append(jnp.where(lane < M, hi, jnp.where(lane >= LANES - M, lo, 0.0)))
    for r in range(z.r):
        for t in range(z.bt):
            ne[NE0 + M + r, t, :, z.c : z.ec] = tiles[r * z.bt + t]
    wx[0:M, :] = jnp.zeros((M, z.ec), F32)
    wx[M + z.r : z.er, :] = jnp.zeros((M, z.ec), F32)
    wx[M : M + z.r, 0 : z.c] = w[...]
    for t in range(z.r // 8):
        wx[M + 8 * t : M + 8 * t + 8, z.c : z.ec] = tiles[z.r * z.bt + t]
    up = tiles[: M * z.bt] + [tiles[z.r * z.bt]]
    down = tiles[(z.r - M) * z.bt : z.r * z.bt] + [tiles[units - 1]]
    up, down = (pack_lanes(x, LANES - M, 2 * M) for x in (up, down))
    lanes = [slice(t * LANES, (t + 1) * LANES) for t in range(z.lt)]
    up += [w[0:8, x] for x in lanes]
    down += [w[z.r - 8 : z.r, x] for x in lanes]
    odd = place[2]
    for v, (u, d) in enumerate(zip(up, down)):
        cor_a[v] = jnp.where(odd == 0, d, u)
        cor_b[v] = jnp.where(odd == 0, u, d)
    sums[...] = jnp.zeros_like(sums)
    first_q(z, ne, edge, [(M, M + z.r - 1)], qx, qy, acc, sums)


def first_q(z, ne, edge, runs, qx, qy, acc, sums):
    across, along = masks(z, edge)
    acc[...] = jnp.zeros_like(acc)

    def band_tile(t, _):
        for lo, hi in runs:
            here = ne[NE0 + lo, t]
            for e in range(lo, hi):
                below_row = ne[NE0 + e + 1, t]
                gx = across(e, below_row - here)
                gy = along(pltpu.roll(here, z.ec - 1, axis=1) - here)
                qx[QX0 + e, t] = gx
                qy[QY0 + e, t] = gy
                acc[e] = acc[e] + (gx * gx + gy * gy)
                here = below_row
        return 0

    lax.fori_loop(0, z.bt, band_tile, 0)
    for lo, hi in runs:
        for e in range(lo, hi):
            sums[e : e + 1, :] = jnp.sum(acc[e], axis=0, keepdims=True)


def masks(z, edge):
    rows = {M - 1: edge[0:1, :], M + z.r - 1: edge[1:2, :]}
    cut = z.c - LANES
    tail = jnp.broadcast_to(edge[2:3, cut : z.ec], (8, z.ec - cut))

    def across(e, d):
        return d * rows[e] if e in rows else d

    def along(d):
        return jnp.concatenate([d[:, 0:cut], d[:, cut : z.ec] * tail], axis=1)

    return across, along


def message_rows(z, k):
    lo, hi = k, z.er - 1 - k
    return lo, hi - lo + (hi - lo) % 2


def message_shape(z, k):
    return (message_rows(z, k)[1] * (z.c // LANES) + 8, LANES)


def write_message(z, k, acc, sums, msg):
    lo, hi = k, z.er - 1 - k
    sums[...] = jnp.zeros_like(sums)
    for e in range(lo, hi):
        sums[e : e + 1, :] = jnp.sum(acc[e], axis=0, keepdims=True)
    pack_message(z, k, sums, msg)


def pack_message(z, k, sums, msg):
    first, n = message_rows(z, k)
    for t in range(z.c // LANES):
        msg[t * n : (t + 1) * n, :] = sums[first : first + n, t * LANES : (t + 1) * LANES]
    halo = [sums[8 * g : 8 * g + 8, z.c : z.ec] for g in range(z.er // 8)]
    msg[n * (z.c // LANES) :, :] = pack_lanes(halo, LANES - M, 2 * M)[0]


def read_scale(z, k, msg_a, msg_b, wx, sums, scale):
    lo, hi = k, z.er - 1 - k
    first, n = message_rows(z, k)
    lane = lane_iota((8, LANES))
    sums[...] = jnp.zeros_like(sums)
    for t in range(z.c // LANES):
        part = slice(t * n, (t + 1) * n)
        sums[first : first + n, t * LANES : (t + 1) * LANES] = msg_a[part, :] + msg_b[part, :]
    packed = msg_a[n * (z.c // LANES) :, :] + msg_b[n * (z.c // LANES) :, :]
    for g in range(z.er // 8):
        got = pltpu.roll(packed, (LANES - M - g * 2 * M) % LANES, axis=1)
        sums[8 * g : 8 * g + 8, z.c : z.ec] = jnp.where((lane < M) | (lane >= LANES - M), got, 0.0)
    w = wx[...]
    sums[...] = w / jnp.maximum(w, jnp.sqrt(1.0 + (SIGMA * SIGMA) * sums[...]))
    for e in range(lo, hi):
        scale[e] = jnp.broadcast_to(sums[e : e + 1, :], (8, z.ec))


def frame_rows(z, place, ne_in, qx_in, qy_in, wx_in, sums_in, edge, a_keep, a_send, b_keep, b_send, cor_a, cor_b, ne, qx, qy, wx, msg, acc, sums):
    core, odd = place[0], place[2]
    lane = lane_iota((8, LANES))
    sub = lax.broadcasted_iota(jnp.int32, (8, z.c), 0)
    per = LANES // (2 * M)
    q4 = z.rest

    for keep, send, first in ((a_keep, a_send, (1 - odd) * (M + z.r)), (b_keep, b_send, odd * (M + z.r))):
        for i in range(M):
            e = NE0 + first + i
            for bt in range(z.ft):
                ne[e, core * z.ft + bt, :, 0 : z.c] = keep[z.ft * i + bt]
                ne[e, (1 - core) * z.ft + bt, :, 0 : z.c] = send[z.ft * i + bt]
            k, s = keep[z.ft * M + i // 2], send[z.ft * M + i // 2]
            k0, s0 = jnp.where(core == 0, k, s), jnp.where(core == 0, s, k)
            if i % 2 == 0:
                s0 = pltpu.roll(s0, q4, axis=0)
            else:
                k0 = pltpu.roll(k0, q4, axis=0)
            ne[e, 2 * z.ft, :, 0 : z.c] = jnp.where(sub < q4, k0, s0)

    n_cor = cor_a.shape[0] - z.lt
    below = [jnp.where(odd == 0, cor_a[v], cor_b[v]) for v in range(n_cor + z.lt)]
    above = [jnp.where(odd == 0, cor_b[v], cor_a[v]) for v in range(n_cor + z.lt)]

    def corner(got, k):
        v, p = divmod(k, per)
        moved = pltpu.roll(got[v], (LANES - M - p * 2 * M) % LANES, axis=1)
        return jnp.where((lane < M) | (lane >= LANES - M), moved, 0.0)

    for r in range(M):
        for t in range(z.bt):
            ne[NE0 + M + z.r + r, t, :, z.c : z.ec] = corner(below, r * z.bt + t)
            ne[NE0 + r, t, :, z.c : z.ec] = corner(above, r * z.bt + t)
    wx[...] = wx_in[...]
    for t in range(z.lt):
        lanes = slice(t * LANES, (t + 1) * LANES)
        wx[M + z.r : z.er, lanes] = below[n_cor + t][0:M]
        wx[0:M, lanes] = above[n_cor + t][8 - M : 8]
    wx[M + z.r : z.er, z.c : z.ec] = corner(below, M * z.bt)[0:M]
    wx[0:M, z.c : z.ec] = corner(above, M * z.bt)[8 - M : 8]
    sums[...] = sums_in[...]
    first_q(z, ne, edge, [(0, M), (M + z.r - 1, z.er - 1)], qx, qy, acc, sums)
    pack_message(z, 0, sums, msg)


CARRY = 1.0 / (1.0 + TAU)
GAIN = TAU / (1.0 + TAU)


def rest_of_update(z, k, ne, u, base):
    def band_tile(t, _):
        for e in range(k + 1, z.er - 1 - k):
            base[NE0 + e, t] = CARRY * u[U0 + e, t] + GAIN * ne[NE0 + e, t]
        return 0

    lax.fori_loop(0, z.bt, band_tile, 0)


def step(z, k, base, wx, edge, u_in, qx_in, qy_in, msg_a, msg_b, u, qx, qy, msg, sums, scale, acc, ubs, pxs, pys):
    lo, hi = k, z.er - 1 - k
    read_scale(z, k, msg_a, msg_b, wx, sums, scale)
    acc[...] = jnp.zeros_like(acc)
    across, along = masks(z, edge)

    def band_tile(t, _):
        px0 = scale[lo] * qx_in[QX0 + lo, t]
        for e in range(lo + 1, hi):
            sc = scale[e]
            px = sc * qx_in[QX0 + e, t]
            py = sc * qy_in[QY0 + e, t]
            div = ((px - px0) + py) - pltpu.roll(py, 1, axis=1)
            old = u_in[(NE0 if k == 0 else U0) + e, t]
            new = (old if k == 0 else base[NE0 + e, t]) + (GAIN * SIGMA) * div
            u[U0 + e, t] = new
            ubs[e] = (new - old) + new
            pxs[e], pys[e] = px, py
            px0 = px
        ub0 = ubs[lo + 1]
        for e in range(lo + 1, hi - 1):
            ub = ubs[e + 1]
            nx = pxs[e] + across(e, ub - ub0)
            ny = pys[e] + along(pltpu.roll(ub0, z.ec - 1, axis=1) - ub0)
            qx[QX0 + e, t] = nx
            qy[QY0 + e, t] = ny
            acc[e] = acc[e] + (nx * nx + ny * ny)
            ub0 = ub
        return 0

    lax.fori_loop(0, z.bt, band_tile, 0)
    write_message(z, k + 1, acc, sums, msg)


def last_step(z, k, own, place, base, wx, qx_in, qy_in, msg_a, msg_b, *refs):
    part = refs[0]
    sums, scale, u = refs[-3:]
    lo, hi = k, z.er - 1 - k
    core = place[0]
    slot = (core if own else 1 - core) * z.ft
    q4 = z.rest
    read_scale(z, k, msg_a, msg_b, wx, sums, scale)

    def band_tile(i, _):
        t = jnp.where(i == z.ft, 2 * z.ft, slot + i)
        px0 = scale[lo] * qx_in[QX0 + lo, t]
        for e in range(lo + 1, hi):
            sc = scale[e]
            px = sc * qx_in[QX0 + e, t]
            py = sc * qy_in[QY0 + e, t]
            div = ((px - px0) + py) - pltpu.roll(py, 1, axis=1)
            new = base[NE0 + e, t] + (GAIN * SIGMA) * div
            u[e - M, i] = new[:, 0 : z.c]
            px0 = px
        return 0

    lax.fori_loop(0, z.ft + 1, band_tile, 0)
    low = (core == 0) if own else (core == 1)
    for r in range(z.r):
        g, q = divmod(r, 8)
        for t in range(z.lt):
            lanes = slice(t * LANES, (t + 1) * LANES)
            run = flat_rows(part, g, t)
            for bt in range(z.ft):
                run[pl.ds(64 * bt + q, 8, stride=8), :] = u[r, bt, :, lanes]
            a, b = u[r, z.ft, 0:q4, lanes], u[r, z.ft, q4:8, lanes]
            run[pl.ds(8 * z.full + q, q4, stride=8), :] = jnp.where(low, a, b)


def write_half(z, own, place, block, *refs):
    out, sem = refs[-2:]
    copies = half_copies(z, place[1] if own else 1 - place[1], out, block, sem, out=True)
    for c in copies:
        c.start()
    for c in copies:
        c.wait()


def local(noisy, weight_map):
    z = Sizes(*noisy.shape)
    n_row, n_col, n_band = (lax.axis_size(a) for a in ("row", "col", "band"))
    chips = n_band // 2
    _, half, _ = here()
    row0 = lax.axis_index("row") * z.r
    col0 = lax.axis_index("col") * (2 * z.c) + half * z.c

    lane = jnp.arange(z.ec)
    gcol = col0 + jnp.where(lane < z.c + LANES // 2, lane, lane - z.ec)
    inner = (gcol >= 0) & (gcol < n_col * 2 * z.c - 1)
    edge = jnp.stack([
        jnp.broadcast_to(row0 > 0, (z.ec,)), jnp.broadcast_to(row0 + z.r < n_row * z.r, (z.ec,)), inner,
    ] + [inner] * 5).astype(F32)

    def at(chip, h):
        return 2 * chip + (h ^ (chip % 2))

    swap = [(i, i ^ 1) for i in range(n_band)]
    pair_a = [(at(c, h), at(c ^ 1, h)) for c in range(chips) for h in range(2)]
    pair_b = [(at(c, h), at((c - 1 + 2 * (c % 2)) % chips, h)) for c in range(chips) for h in range(2)]
    rows_a = [(i, i ^ 1) for i in range(n_row)]
    rows_b = [(i, min(max(i - 1 + 2 * (i % 2), 0), n_row - 1)) for i in range(n_row)]
    across_a = [(i * n_band + b, j * n_band + (b ^ 1)) for i, j in rows_a for b in range(n_band)]
    across_b = [(i * n_band + b, j * n_band + (b ^ 1)) for i, j in rows_b for b in range(n_band)]
    spot = [[(j // 2) * n_band + at(c, j % 2) for j in range(2 * n_col)] for c in range(chips)]
    to_right = [(line[j], line[(j + 1) % len(line)]) for line in spot for j in range(len(line))]
    to_left = [(b, a) for a, b in to_right]

    (edge,) = lax.optimization_barrier((edge,))

    units = z.r * z.bt + z.r // 8
    n_edge = -(-units // (LANES // M))
    n_corner = -(-(M * z.bt + 1) // (LANES // (2 * M)))
    state = (z.er + 4, z.bt, 8, z.ec)
    flat = (z.er, z.ec)
    side = (n_edge, 8, LANES)
    bulk = (z.ft * M + M * z.rest // 8, 8, z.c)
    corner = (n_corner + z.lt, 8, LANES)
    cost = z.er * z.nb * z.ec
    sem = pltpu.SemaphoreType.DMA((z.rg * z.lt,))

    block = (z.lt, z.b, 8, LANES)
    sem_g = pltpu.SemaphoreType.DMA((z.lt,))
    cube, weights = (pltpu.with_memory_space_constraint(x, pltpu.HBM) for x in (noisy, weight_map))
    parts, far = [], []
    for name, same, cross in (("a", rows_a, across_a), ("b", rows_b, across_b)):
        b = name == "b"
        keep, send, msg_keep, msg_send, *w = call(
            lambda *a, b=b: split(z, b, here(), *a), [block, block, bulk, bulk] + [(z.r, z.c)] * b,
            [cube, edge] + [weights] * b, scratch=[sem_g, sem_g] + [pltpu.SemaphoreType.DMA] * b,
            hbm_in=(0, 2), flops=cost,
        )
        far.append(lax.ppermute(msg_keep, "row", same))
        far.append(lax.ppermute(msg_send, ("row", "band"), cross))
        parts += [keep, lax.ppermute(send, "band", swap)]
    (w,) = w
    ne, col_l, col_r = call(
        lambda *a: assemble(z, here(), *a), [state, side, side], [*parts, w, edge], flops=cost
    )
    from_r = lax.ppermute(col_l, ("col", "band"), to_left)
    from_l = lax.ppermute(col_r, ("col", "band"), to_right)
    acc = pltpu.VMEM((z.er, 8, z.ec), F32)
    one = pltpu.VMEM(flat, F32)
    ne, wx, qx, qy, sums, cor_a, cor_b = call(
        lambda *a: frame_cols(z, here(), *a), [state, flat, state, state, flat, corner, corner],
        [ne, w, edge, from_r, from_l], aliases={0: 0}, scratch=[acc], flops=5 * cost,
    )
    cor_a = lax.ppermute(cor_a, "row", rows_a)
    cor_b = lax.ppermute(cor_b, "row", rows_b)
    ne, qx, qy, wx, msg = call(
        lambda *a: frame_rows(z, here(), *a), [state, state, state, flat, message_shape(z, 0)],
        [ne, qx, qy, wx, sums, edge, *far, cor_a, cor_b],
        aliases={0: 0, 1: 1, 2: 2}, scratch=[acc, one], flops=5 * cost,
    )
    u = base = ne
    for k in range(ITERS):
        msg = msg + lax.ppermute(msg, "band", pair_a)
        other = lax.ppermute(msg, "band", pair_b)
        if k > 0:
            (base,) = call(lambda *a, k=k: rest_of_update(z, k, *a), [state], [ne, u], flops=cost)
        if k < ITERS - 1:
            u, qx, qy, msg = call(
                lambda *a, k=k: step(z, k, *a), [state, state, state, message_shape(z, k + 1)],
                [base, wx, edge, u, qx, qy, msg, other], scratch=[one, acc, acc, acc, acc, acc], flops=20 * cost,
            )
    last = [base, wx, qx, qy, msg, other]
    room = [one, acc, pltpu.VMEM((z.r, z.ft + 1, 8, z.c), F32)]
    (send,) = call(lambda *a: last_step(z, ITERS - 1, False, here(), *a), [z.block], last, scratch=room, flops=5 * cost)
    recv = lax.ppermute(send, "band", swap)
    (keep,) = call(lambda *a: last_step(z, ITERS - 1, True, here(), *a), [z.block], last, scratch=room, flops=5 * cost)
    (out,) = call(
        lambda *a: write_half(z, True, here(), *a), [noisy.shape], [keep], scratch=[sem], hbm_out=(0,), flops=cost
    )
    (out,) = call(
        lambda *a: write_half(z, False, here(), *a), [noisy.shape], [recv, out],
        aliases={1: 0}, scratch=[sem], hbm_in=(1,), hbm_out=(0,), flops=cost,
    )
    return out


def solution(mesh):
    placed = (P("band", "row", "col"), P("row", "col"))
    return jax.shard_map(local, mesh=mesh, in_specs=placed, out_specs=P("band", "row", "col"), check_vma=False)
```

```python
import jax
import jax.numpy as jnp
from jax import lax
from jax.experimental import pallas as pl
from jax.experimental.pallas import tpu as pltpu
from jax.sharding import PartitionSpec as P


ITERS = 4
M = ITERS
LANES = 128
SIGMA = 0.35
TAU = 0.35


F32 = jnp.float32
U0, QX0, QY0, NE0 = range(4)
VM = pl.BlockSpec(memory_space=pltpu.VMEM)
SM = pl.BlockSpec(memory_space=pltpu.SMEM)
HB = pl.BlockSpec(memory_space=pltpu.HBM)
PARAMS = pltpu.CompilerParams(vmem_limit_bytes=8 * 1024 * 1024)


def call(body, outs, ins, n_smem=0, aliases=None, scratch=(), flops=0, hbm_in=(), hbm_out=()):
    in_specs = [SM] * n_smem + [VM] * (len(ins) - n_smem)
    return pl.pallas_call(
        body,
        out_shape=[(pltpu.HBM if i in hbm_out else pltpu.VMEM)(s, F32) for i, s in enumerate(outs)],
        in_specs=[HB if i in hbm_in else spec for i, spec in enumerate(in_specs)],
        out_specs=[HB if i in hbm_out else VM for i in range(len(outs))],
        scratch_shapes=list(scratch),
        input_output_aliases=aliases or {},
        compiler_params=PARAMS,
        cost_estimate=pl.CostEstimate(flops=flops, bytes_accessed=0, transcendentals=0),
    )(*ins)


def here():
    band = lax.axis_index("band")
    core = lax.rem(band, 2)
    return core, core ^ lax.rem(lax.div(band, 2), 2), lax.rem(lax.axis_index("row"), 2)


def lane_iota(shape):
    return lax.broadcasted_iota(jnp.int32, shape, len(shape) - 1)


class Sizes:
    def __init__(self, bands, rows, cols):
        self.b = bands
        self.nb = 2 * bands
        self.bt = self.nb // 8
        self.r = rows
        self.c = cols // 2
        self.er = rows + 2 * M
        self.ec = self.c + LANES
        self.full = self.b // 8 * 8
        self.rest = self.b - self.full
        self.ft = self.full // 8
        self.rg = rows // 8
        self.lt = self.c // LANES
        self.block = (self.rg, self.lt, self.b, 8, LANES)


def pack_lanes(tiles, first, width):
    per = LANES // width
    lane = lane_iota((8, LANES))
    out = []
    for v in range(0, len(tiles), per):
        acc = None
        for p, tile in enumerate(tiles[v : v + per]):
            moved = pltpu.roll(tile, (p * width - first) % LANES, axis=1)
            acc = moved if acc is None else jnp.where(lane // width == p, moved, acc)
        out.append(acc)
    return out


def flat_rows(ref, *at):
    tile = ref.at[at]
    return tile.reshape(tile.shape[0] * 8, LANES)


def half_copies(z, half, array, block, sem, group=None, out=False):
    copies = []
    for g in range(z.rg) if group is None else (None,):
        rows = pl.ds(8 * g, 8) if group is None else pl.ds(pl.multiple_of(group * 8, 8), 8)
        for t in range(z.lt):
            lanes = pl.ds(pl.multiple_of(half * z.c + t * LANES, LANES), LANES)
            ends = [array.at[:, rows, lanes], block.at[t] if group is not None else block.at[g, t]]
            copies.append(pltpu.make_async_copy(*(ends[::-1] if out else ends), sem.at[(g or 0) * z.lt + t]))
    return copies


def split(z, facing_b, place, noisy, edge, *refs):
    weights, (keep, send, msg_keep, msg_send), more = refs[0], refs[facing_b : facing_b + 4], refs[facing_b + 4 :]
    sem_k, sem_s = more[facing_b : facing_b + 2]
    half, odd = place[1], place[2]
    group = odd if facing_b else 1 - odd
    copies = half_copies(z, half, noisy, keep, sem_k, group) + half_copies(z, 1 - half, noisy, send, sem_s, group)
    if facing_b:
        lanes = pl.ds(pl.multiple_of(half * z.c, LANES), z.c)
        copies.append(pltpu.make_async_copy(weights.at[:, lanes], more[0], more[3]))
    for c in copies:
        c.start()
    for c in copies:
        c.wait()

    def rows(block, first, msg):
        for i in range(M):
            q = first + i
            for t in range(z.lt):
                run = flat_rows(block, t)
                lanes = slice(t * LANES, (t + 1) * LANES)
                for bt in range(z.ft):
                    msg[z.ft * i + bt, :, lanes] = run[pl.ds(64 * bt + q, 8, stride=8), :]
                at = z.rest * (i % 2)
                msg[z.ft * M + i // 2, at : at + z.rest, lanes] = run[pl.ds(8 * z.full + q, z.rest, stride=8), :]

    @pl.when(group == 0)
    def _():
        rows(keep, 0, msg_keep)
        rows(send, 0, msg_send)

    @pl.when(group == 1)
    def _():
        rows(keep, 8 - M, msg_keep)
        rows(send, 8 - M, msg_send)


def assemble(z, place, keep_a, send_a, keep_b, send_b, w, edge, ne, col_l, col_r):
    core, odd = place[0], place[2]
    q4 = z.rest
    for keep, recv, group in ((keep_a, send_a, 1 - odd), (keep_b, send_b, odd)):
        for q in range(8):
            e = NE0 + M + 8 * group + q
            for t in range(z.lt):
                lanes = slice(t * LANES, (t + 1) * LANES)
                mine, other = flat_rows(keep, t), flat_rows(recv, t)
                for bt in range(z.ft):
                    ne[e, core * z.ft + bt, :, lanes] = mine[pl.ds(64 * bt + q, 8, stride=8), :]
                    ne[e, (1 - core) * z.ft + bt, :, lanes] = other[pl.ds(64 * bt + q, 8, stride=8), :]
                a = mine[pl.ds(8 * z.full + q, q4, stride=8), :]
                b = other[pl.ds(8 * z.full + q, q4, stride=8), :]
                ne[e, 2 * z.ft, 0:q4, lanes] = jnp.where(core == 0, a, b)
                ne[e, 2 * z.ft, q4:8, lanes] = jnp.where(core == 0, b, a)
    last = slice(z.c - LANES, z.c)
    left = [ne[NE0 + M + r, t, :, 0:LANES] for r in range(z.r) for t in range(z.bt)]
    left += [w[8 * t : 8 * t + 8, 0:LANES] for t in range(z.r // 8)]
    right = [ne[NE0 + M + r, t, :, last] for r in range(z.r) for t in range(z.bt)]
    right += [w[8 * t : 8 * t + 8, last] for t in range(z.r // 8)]
    for v, tile in enumerate(pack_lanes(left, 0, M)):
        col_l[v] = tile
    for v, tile in enumerate(pack_lanes(right, LANES - M, M)):
        col_r[v] = tile


def frame_cols(z, place, ne_in, w, edge, from_r, from_l, ne, wx, qx, qy, sums, cor_a, cor_b, acc):
    lane = lane_iota((8, LANES))
    per = LANES // M
    units = z.r * z.bt + z.r // 8
    tiles = []
    for k in range(units):
        v, p = divmod(k, per)
        hi = pltpu.roll(from_r[v], (-p * M) % LANES, axis=1)
        lo = pltpu.roll(from_l[v], (LANES - M - p * M) % LANES, axis=1)
        tiles.append(jnp.where(lane < M, hi, jnp.where(lane >= LANES - M, lo, 0.0)))
    for r in range(z.r):
        for t in range(z.bt):
            ne[NE0 + M + r, t, :, z.c : z.ec] = tiles[r * z.bt + t]
    wx[0:M, :] = jnp.zeros((M, z.ec), F32)
    wx[M + z.r : z.er, :] = jnp.zeros((M, z.ec), F32)
    wx[M : M + z.r, 0 : z.c] = w[...]
    for t in range(z.r // 8):
        wx[M + 8 * t : M + 8 * t + 8, z.c : z.ec] = tiles[z.r * z.bt + t]
    up = tiles[: M * z.bt] + [tiles[z.r * z.bt]]
    down = tiles[(z.r - M) * z.bt : z.r * z.bt] + [tiles[units - 1]]
    up, down = (pack_lanes(x, LANES - M, 2 * M) for x in (up, down))
    lanes = [slice(t * LANES, (t + 1) * LANES) for t in range(z.lt)]
    up += [w[0:8, x] for x in lanes]
    down += [w[z.r - 8 : z.r, x] for x in lanes]
    odd = place[2]
    for v, (u, d) in enumerate(zip(up, down)):
        cor_a[v] = jnp.where(odd == 0, d, u)
        cor_b[v] = jnp.where(odd == 0, u, d)
    sums[...] = jnp.zeros_like(sums)
    first_q(z, ne, edge, [(M, M + z.r - 1)], qx, qy, acc, sums)


def first_q(z, ne, edge, runs, qx, qy, acc, sums):
    across, along = masks(z, edge)
    acc[...] = jnp.zeros_like(acc)

    def band_tile(t, _):
        for lo, hi in runs:
            here = ne[NE0 + lo, t]
            for e in range(lo, hi):
                below_row = ne[NE0 + e + 1, t]
                gx = across(e, below_row - here)
                gy = along(pltpu.roll(here, z.ec - 1, axis=1) - here)
                qx[QX0 + e, t] = gx
                qy[QY0 + e, t] = gy
                acc[e] = acc[e] + (gx * gx + gy * gy)
                here = below_row
        return 0

    lax.fori_loop(0, z.bt, band_tile, 0)
    for lo, hi in runs:
        for e in range(lo, hi):
            sums[e : e + 1, :] = jnp.sum(acc[e], axis=0, keepdims=True)


def masks(z, edge):
    rows = {M - 1: edge[0:1, :], M + z.r - 1: edge[1:2, :]}
    cut = z.c - LANES
    tail = jnp.broadcast_to(edge[2:3, cut : z.ec], (8, z.ec - cut))

    def across(e, d):
        return d * rows[e] if e in rows else d

    def along(d):
        return jnp.concatenate([d[:, 0:cut], d[:, cut : z.ec] * tail], axis=1)

    return across, along


def message_rows(z, k):
    lo, hi = k, z.er - 1 - k
    return lo, hi - lo + (hi - lo) % 2


def message_shape(z, k):
    return (message_rows(z, k)[1] * (z.c // LANES) + 8, LANES)


def write_message(z, k, acc, sums, msg):
    lo, hi = k, z.er - 1 - k
    sums[...] = jnp.zeros_like(sums)
    for e in range(lo, hi):
        sums[e : e + 1, :] = jnp.sum(acc[e], axis=0, keepdims=True)
    pack_message(z, k, sums, msg)


def pack_message(z, k, sums, msg):
    first, n = message_rows(z, k)
    for t in range(z.c // LANES):
        msg[t * n : (t + 1) * n, :] = sums[first : first + n, t * LANES : (t + 1) * LANES]
    halo = [sums[8 * g : 8 * g + 8, z.c : z.ec] for g in range(z.er // 8)]
    msg[n * (z.c // LANES) :, :] = pack_lanes(halo, LANES - M, 2 * M)[0]


def read_scale(z, k, msg_a, msg_b, wx, sums, scale):
    lo, hi = k, z.er - 1 - k
    first, n = message_rows(z, k)
    lane = lane_iota((8, LANES))
    sums[...] = jnp.zeros_like(sums)
    for t in range(z.c // LANES):
        part = slice(t * n, (t + 1) * n)
        sums[first : first + n, t * LANES : (t + 1) * LANES] = msg_a[part, :] + msg_b[part, :]
    packed = msg_a[n * (z.c // LANES) :, :] + msg_b[n * (z.c // LANES) :, :]
    for g in range(z.er // 8):
        got = pltpu.roll(packed, (LANES - M - g * 2 * M) % LANES, axis=1)
        sums[8 * g : 8 * g + 8, z.c : z.ec] = jnp.where((lane < M) | (lane >= LANES - M), got, 0.0)
    w = wx[...]
    sums[...] = w / jnp.maximum(w, jnp.sqrt(1.0 + (SIGMA * SIGMA) * sums[...]))
    for e in range(lo, hi):
        scale[e] = jnp.broadcast_to(sums[e : e + 1, :], (8, z.ec))


def frame_rows(z, place, ne_in, qx_in, qy_in, wx_in, sums_in, edge, a_keep, a_send, b_keep, b_send, cor_a, cor_b, ne, qx, qy, wx, msg, acc, sums):
    core, odd = place[0], place[2]
    lane = lane_iota((8, LANES))
    sub = lax.broadcasted_iota(jnp.int32, (8, z.c), 0)
    per = LANES // (2 * M)
    q4 = z.rest

    for keep, send, first in ((a_keep, a_send, (1 - odd) * (M + z.r)), (b_keep, b_send, odd * (M + z.r))):
        for i in range(M):
            e = NE0 + first + i
            for bt in range(z.ft):
                ne[e, core * z.ft + bt, :, 0 : z.c] = keep[z.ft * i + bt]
                ne[e, (1 - core) * z.ft + bt, :, 0 : z.c] = send[z.ft * i + bt]
            k, s = keep[z.ft * M + i // 2], send[z.ft * M + i // 2]
            k0, s0 = jnp.where(core == 0, k, s), jnp.where(core == 0, s, k)
            if i % 2 == 0:
                s0 = pltpu.roll(s0, q4, axis=0)
            else:
                k0 = pltpu.roll(k0, q4, axis=0)
            ne[e, 2 * z.ft, :, 0 : z.c] = jnp.where(sub < q4, k0, s0)

    n_cor = cor_a.shape[0] - z.lt
    below = [jnp.where(odd == 0, cor_a[v], cor_b[v]) for v in range(n_cor + z.lt)]
    above = [jnp.where(odd == 0, cor_b[v], cor_a[v]) for v in range(n_cor + z.lt)]

    def corner(got, k):
        v, p = divmod(k, per)
        moved = pltpu.roll(got[v], (LANES - M - p * 2 * M) % LANES, axis=1)
        return jnp.where((lane < M) | (lane >= LANES - M), moved, 0.0)

    for r in range(M):
        for t in range(z.bt):
            ne[NE0 + M + z.r + r, t, :, z.c : z.ec] = corner(below, r * z.bt + t)
            ne[NE0 + r, t, :, z.c : z.ec] = corner(above, r * z.bt + t)
    wx[...] = wx_in[...]
    for t in range(z.lt):
        lanes = slice(t * LANES, (t + 1) * LANES)
        wx[M + z.r : z.er, lanes] = below[n_cor + t][0:M]
        wx[0:M, lanes] = above[n_cor + t][8 - M : 8]
    wx[M + z.r : z.er, z.c : z.ec] = corner(below, M * z.bt)[0:M]
    wx[0:M, z.c : z.ec] = corner(above, M * z.bt)[8 - M : 8]
    sums[...] = sums_in[...]
    first_q(z, ne, edge, [(0, M), (M + z.r - 1, z.er - 1)], qx, qy, acc, sums)
    pack_message(z, 0, sums, msg)


CARRY = 1.0 / (1.0 + TAU)
GAIN = TAU / (1.0 + TAU)


def rest_of_update(z, k, ne, u, base):
    def band_tile(t, _):
        for e in range(k + 1, z.er - 1 - k):
            base[NE0 + e, t] = CARRY * u[U0 + e, t] + GAIN * ne[NE0 + e, t]
        return 0

    lax.fori_loop(0, z.bt, band_tile, 0)


def step(z, k, base, wx, edge, u_in, qx_in, qy_in, msg_a, msg_b, u, qx, qy, msg, sums, scale, acc, ubs, pxs, pys):
    lo, hi = k, z.er - 1 - k
    read_scale(z, k, msg_a, msg_b, wx, sums, scale)
    acc[...] = jnp.zeros_like(acc)
    across, along = masks(z, edge)

    def band_tile(t, _):
        px0 = scale[lo] * qx_in[QX0 + lo, t]
        for e in range(lo + 1, hi):
            sc = scale[e]
            px = sc * qx_in[QX0 + e, t]
            py = sc * qy_in[QY0 + e, t]
            div = ((px - px0) + py) - pltpu.roll(py, 1, axis=1)
            old = u_in[(NE0 if k == 0 else U0) + e, t]
            new = (old if k == 0 else base[NE0 + e, t]) + (GAIN * SIGMA) * div
            u[U0 + e, t] = new
            ubs[e] = (new - old) + new
            pxs[e], pys[e] = px, py
            px0 = px
        ub0 = ubs[lo + 1]
        for e in range(lo + 1, hi - 1):
            ub = ubs[e + 1]
            nx = pxs[e] + across(e, ub - ub0)
            ny = pys[e] + along(pltpu.roll(ub0, z.ec - 1, axis=1) - ub0)
            qx[QX0 + e, t] = nx
            qy[QY0 + e, t] = ny
            acc[e] = acc[e] + (nx * nx + ny * ny)
            ub0 = ub
        return 0

    lax.fori_loop(0, z.bt, band_tile, 0)
    write_message(z, k + 1, acc, sums, msg)


def last_step(z, k, own, place, base, wx, qx_in, qy_in, msg_a, msg_b, *refs):
    part = refs[0]
    sums, scale, u = refs[-3:]
    lo, hi = k, z.er - 1 - k
    core = place[0]
    slot = (core if own else 1 - core) * z.ft
    q4 = z.rest
    read_scale(z, k, msg_a, msg_b, wx, sums, scale)

    def band_tile(i, _):
        t = jnp.where(i == z.ft, 2 * z.ft, slot + i)
        px0 = scale[lo] * qx_in[QX0 + lo, t]
        for e in range(lo + 1, hi):
            sc = scale[e]
            px = sc * qx_in[QX0 + e, t]
            py = sc * qy_in[QY0 + e, t]
            div = ((px - px0) + py) - pltpu.roll(py, 1, axis=1)
            new = base[NE0 + e, t] + (GAIN * SIGMA) * div
            u[e - M, i] = new[:, 0 : z.c]
            px0 = px
        return 0

    lax.fori_loop(0, z.ft + 1, band_tile, 0)
    low = (core == 0) if own else (core == 1)
    for r in range(z.r):
        g, q = divmod(r, 8)
        for t in range(z.lt):
            lanes = slice(t * LANES, (t + 1) * LANES)
            run = flat_rows(part, g, t)
            for bt in range(z.ft):
                run[pl.ds(64 * bt + q, 8, stride=8), :] = u[r, bt, :, lanes]
            a, b = u[r, z.ft, 0:q4, lanes], u[r, z.ft, q4:8, lanes]
            run[pl.ds(8 * z.full + q, q4, stride=8), :] = jnp.where(low, a, b)


def write_half(z, own, place, block, *refs):
    out, sem = refs[-2:]
    copies = half_copies(z, place[1] if own else 1 - place[1], out, block, sem, out=True)
    for c in copies:
        c.start()
    for c in copies:
        c.wait()


def local(noisy, weight_map):
    z = Sizes(*noisy.shape)
    n_row, n_col, n_band = (lax.axis_size(a) for a in ("row", "col", "band"))
    chips = n_band // 2
    _, half, _ = here()
    row0 = lax.axis_index("row") * z.r
    col0 = lax.axis_index("col") * (2 * z.c) + half * z.c

    lane = jnp.arange(z.ec)
    gcol = col0 + jnp.where(lane < z.c + LANES // 2, lane, lane - z.ec)
    inner = (gcol >= 0) & (gcol < n_col * 2 * z.c - 1)
    edge = jnp.stack([
        jnp.broadcast_to(row0 > 0, (z.ec,)), jnp.broadcast_to(row0 + z.r < n_row * z.r, (z.ec,)), inner,
    ] + [inner] * 5).astype(F32)

    def at(chip, h):
        return 2 * chip + (h ^ (chip % 2))

    swap = [(i, i ^ 1) for i in range(n_band)]
    pair_a = [(at(c, h), at(c ^ 1, h)) for c in range(chips) for h in range(2)]
    pair_b = [(at(c, h), at((c - 1 + 2 * (c % 2)) % chips, h)) for c in range(chips) for h in range(2)]
    rows_a = [(i, i ^ 1) for i in range(n_row)]
    rows_b = [(i, min(max(i - 1 + 2 * (i % 2), 0), n_row - 1)) for i in range(n_row)]
    across_a = [(i * n_band + b, j * n_band + (b ^ 1)) for i, j in rows_a for b in range(n_band)]
    across_b = [(i * n_band + b, j * n_band + (b ^ 1)) for i, j in rows_b for b in range(n_band)]
    spot = [[(j // 2) * n_band + at(c, j % 2) for j in range(2 * n_col)] for c in range(chips)]
    to_right = [(line[j], line[(j + 1) % len(line)]) for line in spot for j in range(len(line))]
    to_left = [(b, a) for a, b in to_right]

    (edge,) = lax.optimization_barrier((edge,))

    units = z.r * z.bt + z.r // 8
    n_edge = -(-units // (LANES // M))
    n_corner = -(-(M * z.bt + 1) // (LANES // (2 * M)))
    state = (z.er + 4, z.bt, 8, z.ec)
    flat = (z.er, z.ec)
    side = (n_edge, 8, LANES)
    bulk = (z.ft * M + M * z.rest // 8, 8, z.c)
    corner = (n_corner + z.lt, 8, LANES)
    cost = z.er * z.nb * z.ec
    sem = pltpu.SemaphoreType.DMA((z.rg * z.lt,))

    block = (z.lt, z.b, 8, LANES)
    sem_g = pltpu.SemaphoreType.DMA((z.lt,))
    cube, weights = (pltpu.with_memory_space_constraint(x, pltpu.HBM) for x in (noisy, weight_map))
    parts, far = [], []
    for name, same, cross in (("a", rows_a, across_a), ("b", rows_b, across_b)):
        b = name == "b"
        keep, send, msg_keep, msg_send, *w = call(
            lambda *a, b=b: split(z, b, here(), *a), [block, block, bulk, bulk] + [(z.r, z.c)] * b,
            [cube, edge] + [weights] * b, scratch=[sem_g, sem_g] + [pltpu.SemaphoreType.DMA] * b,
            hbm_in=(0, 2), flops=cost,
        )
        far.append(lax.ppermute(msg_keep, "row", same))
        far.append(lax.ppermute(msg_send, ("row", "band"), cross))
        parts += [keep, lax.ppermute(send, "band", swap)]
    (w,) = w
    ne, col_l, col_r = call(
        lambda *a: assemble(z, here(), *a), [state, side, side], [*parts, w, edge], flops=cost
    )
    from_r = lax.ppermute(col_l, ("col", "band"), to_left)
    from_l = lax.ppermute(col_r, ("col", "band"), to_right)
    acc = pltpu.VMEM((z.er, 8, z.ec), F32)
    one = pltpu.VMEM(flat, F32)
    ne, wx, qx, qy, sums, cor_a, cor_b = call(
        lambda *a: frame_cols(z, here(), *a), [state, flat, state, state, flat, corner, corner],
        [ne, w, edge, from_r, from_l], aliases={0: 0}, scratch=[acc], flops=5 * cost,
    )
    cor_a = lax.ppermute(cor_a, "row", rows_a)
    cor_b = lax.ppermute(cor_b, "row", rows_b)
    ne, qx, qy, wx, msg = call(
        lambda *a: frame_rows(z, here(), *a), [state, state, state, flat, message_shape(z, 0)],
        [ne, qx, qy, wx, sums, edge, *far, cor_a, cor_b],
        aliases={0: 0, 1: 1, 2: 2}, scratch=[acc, one], flops=5 * cost,
    )
    u = base = ne
    for k in range(ITERS):
        pairs = (pair_a, pair_b) if k % 2 == 0 else (pair_b, pair_a)
        msg = msg + lax.ppermute(msg, "band", pairs[0])
        other = lax.ppermute(msg, "band", pairs[1])
        if k > 0:
            (base,) = call(lambda *a, k=k: rest_of_update(z, k, *a), [state], [ne, u], flops=cost)
        if k < ITERS - 1:
            u, qx, qy, msg = call(
                lambda *a, k=k: step(z, k, *a), [state, state, state, message_shape(z, k + 1)],
                [base, wx, edge, u, qx, qy, msg, other], scratch=[one, acc, acc, acc, acc, acc], flops=20 * cost,
            )
    last = [base, wx, qx, qy, msg, other]
    room = [one, acc, pltpu.VMEM((z.r, z.ft + 1, 8, z.c), F32)]
    (send,) = call(lambda *a: last_step(z, ITERS - 1, False, here(), *a), [z.block], last, scratch=room, flops=5 * cost)
    recv = lax.ppermute(send, "band", swap)
    (keep,) = call(lambda *a: last_step(z, ITERS - 1, True, here(), *a), [z.block], last, scratch=room, flops=5 * cost)
    (out,) = call(
        lambda *a: write_half(z, True, here(), *a), [noisy.shape], [keep], scratch=[sem], hbm_out=(0,), flops=cost
    )
    (out,) = call(
        lambda *a: write_half(z, False, here(), *a), [noisy.shape], [recv, out],
        aliases={1: 0}, scratch=[sem], hbm_in=(1,), hbm_out=(0,), flops=cost,
    )
    return out


def solution(mesh):
    placed = (P("band", "row", "col"), P("row", "col"))
    return jax.shard_map(local, mesh=mesh, in_specs=placed, out_specs=P("band", "row", "col"), check_vma=False)
```

```python
import jax
import jax.numpy as jnp
from jax import lax
from jax.experimental import pallas as pl
from jax.experimental.pallas import tpu as pltpu
from jax.sharding import PartitionSpec as P


ITERS = 4
M = ITERS
LANES = 128
SIGMA = 0.35
TAU = 0.35


F32 = jnp.float32
U0, QX0, QY0, NE0 = range(4)
VM = pl.BlockSpec(memory_space=pltpu.VMEM)
SM = pl.BlockSpec(memory_space=pltpu.SMEM)
HB = pl.BlockSpec(memory_space=pltpu.HBM)
PARAMS = pltpu.CompilerParams(vmem_limit_bytes=8 * 1024 * 1024)


def call(body, outs, ins, n_smem=0, aliases=None, scratch=(), flops=0, hbm_in=(), hbm_out=()):
    in_specs = [SM] * n_smem + [VM] * (len(ins) - n_smem)
    return pl.pallas_call(
        body,
        out_shape=[(pltpu.HBM if i in hbm_out else pltpu.VMEM)(s, F32) for i, s in enumerate(outs)],
        in_specs=[HB if i in hbm_in else spec for i, spec in enumerate(in_specs)],
        out_specs=[HB if i in hbm_out else VM for i in range(len(outs))],
        scratch_shapes=list(scratch),
        input_output_aliases=aliases or {},
        compiler_params=PARAMS,
        cost_estimate=pl.CostEstimate(flops=flops, bytes_accessed=0, transcendentals=0),
    )(*ins)


def here():
    band = lax.axis_index("band")
    core = lax.rem(band, 2)
    return core, core ^ lax.rem(lax.div(band, 2), 2), lax.rem(lax.axis_index("row"), 2)


def lane_iota(shape):
    return lax.broadcasted_iota(jnp.int32, shape, len(shape) - 1)


class Sizes:
    def __init__(self, bands, rows, cols):
        self.b = bands
        self.nb = 2 * bands
        self.bt = self.nb // 8
        self.r = rows
        self.c = cols // 2
        self.er = rows + 2 * M
        self.ec = self.c + LANES
        self.full = self.b // 8 * 8
        self.rest = self.b - self.full
        self.ft = self.full // 8
        self.rg = rows // 8
        self.lt = self.c // LANES
        self.block = (self.rg, self.lt, self.b, 8, LANES)


def pack_lanes(tiles, first, width):
    per = LANES // width
    lane = lane_iota((8, LANES))
    out = []
    for v in range(0, len(tiles), per):
        acc = None
        for p, tile in enumerate(tiles[v : v + per]):
            moved = pltpu.roll(tile, (p * width - first) % LANES, axis=1)
            acc = moved if acc is None else jnp.where(lane // width == p, moved, acc)
        out.append(acc)
    return out


def flat_rows(ref, *at):
    tile = ref.at[at]
    return tile.reshape(tile.shape[0] * 8, LANES)


def half_copies(z, half, array, block, sem, group=None, out=False):
    copies = []
    for g in range(z.rg) if group is None else (None,):
        rows = pl.ds(8 * g, 8) if group is None else pl.ds(pl.multiple_of(group * 8, 8), 8)
        for t in range(z.lt):
            lanes = pl.ds(pl.multiple_of(half * z.c + t * LANES, LANES), LANES)
            ends = [array.at[:, rows, lanes], block.at[t] if group is not None else block.at[g, t]]
            copies.append(pltpu.make_async_copy(*(ends[::-1] if out else ends), sem.at[(g or 0) * z.lt + t]))
    return copies


def split(z, facing_b, place, noisy, *refs):
    weights, (keep, send, msg_keep, msg_send), more = refs[0], refs[facing_b : facing_b + 4], refs[facing_b + 4 :]
    sem_k, sem_s = more[facing_b : facing_b + 2]
    half, odd = place[1], place[2]
    group = odd if facing_b else 1 - odd
    copies = half_copies(z, half, noisy, keep, sem_k, group) + half_copies(z, 1 - half, noisy, send, sem_s, group)
    if facing_b:
        lanes = pl.ds(pl.multiple_of(half * z.c, LANES), z.c)
        copies.append(pltpu.make_async_copy(weights.at[:, lanes], more[0], more[3]))
    for c in copies:
        c.start()
    for c in copies:
        c.wait()

    def rows(block, first, msg):
        for i in range(M):
            q = first + i
            for t in range(z.lt):
                run = flat_rows(block, t)
                lanes = slice(t * LANES, (t + 1) * LANES)
                for bt in range(z.ft):
                    msg[z.ft * i + bt, :, lanes] = run[pl.ds(64 * bt + q, 8, stride=8), :]
                at = z.rest * (i % 2)
                msg[z.ft * M + i // 2, at : at + z.rest, lanes] = run[pl.ds(8 * z.full + q, z.rest, stride=8), :]

    @pl.when(group == 0)
    def _():
        rows(keep, 0, msg_keep)
        rows(send, 0, msg_send)

    @pl.when(group == 1)
    def _():
        rows(keep, 8 - M, msg_keep)
        rows(send, 8 - M, msg_send)


def assemble(z, place, keep_a, send_a, keep_b, send_b, w, ne, col_l, col_r):
    core, odd = place[0], place[2]
    q4 = z.rest
    for keep, recv, group in ((keep_a, send_a, 1 - odd), (keep_b, send_b, odd)):
        for q in range(8):
            e = NE0 + M + 8 * group + q
            for t in range(z.lt):
                lanes = slice(t * LANES, (t + 1) * LANES)
                mine, other = flat_rows(keep, t), flat_rows(recv, t)
                for bt in range(z.ft):
                    ne[e, core * z.ft + bt, :, lanes] = mine[pl.ds(64 * bt + q, 8, stride=8), :]
                    ne[e, (1 - core) * z.ft + bt, :, lanes] = other[pl.ds(64 * bt + q, 8, stride=8), :]
                a = mine[pl.ds(8 * z.full + q, q4, stride=8), :]
                b = other[pl.ds(8 * z.full + q, q4, stride=8), :]
                ne[e, 2 * z.ft, 0:q4, lanes] = jnp.where(core == 0, a, b)
                ne[e, 2 * z.ft, q4:8, lanes] = jnp.where(core == 0, b, a)
    last = slice(z.c - LANES, z.c)
    left = [ne[NE0 + M + r, t, :, 0:LANES] for r in range(z.r) for t in range(z.bt)]
    left += [w[8 * t : 8 * t + 8, 0:LANES] for t in range(z.r // 8)]
    right = [ne[NE0 + M + r, t, :, last] for r in range(z.r) for t in range(z.bt)]
    right += [w[8 * t : 8 * t + 8, last] for t in range(z.r // 8)]
    for v, tile in enumerate(pack_lanes(left, 0, M)):
        col_l[v] = tile
    for v, tile in enumerate(pack_lanes(right, LANES - M, M)):
        col_r[v] = tile


def frame_cols(z, place, ne_in, w, from_r, from_l, ne, wx, qx, qy, sums, cor_a, cor_b, acc):
    lane = lane_iota((8, LANES))
    per = LANES // M
    units = z.r * z.bt + z.r // 8
    tiles = []
    for k in range(units):
        v, p = divmod(k, per)
        hi = pltpu.roll(from_r[v], (-p * M) % LANES, axis=1)
        lo = pltpu.roll(from_l[v], (LANES - M - p * M) % LANES, axis=1)
        tiles.append(jnp.where(lane < M, hi, jnp.where(lane >= LANES - M, lo, 0.0)))
    for r in range(z.r):
        for t in range(z.bt):
            ne[NE0 + M + r, t, :, z.c : z.ec] = tiles[r * z.bt + t]
    wx[0:M, :] = jnp.zeros((M, z.ec), F32)
    wx[M + z.r : z.er, :] = jnp.zeros((M, z.ec), F32)
    wx[M : M + z.r, 0 : z.c] = w[...]
    for t in range(z.r // 8):
        wx[M + 8 * t : M + 8 * t + 8, z.c : z.ec] = tiles[z.r * z.bt + t]
    up = tiles[: M * z.bt] + [tiles[z.r * z.bt]]
    down = tiles[(z.r - M) * z.bt : z.r * z.bt] + [tiles[units - 1]]
    up, down = (pack_lanes(x, LANES - M, 2 * M) for x in (up, down))
    lanes = [slice(t * LANES, (t + 1) * LANES) for t in range(z.lt)]
    up += [w[0:8, x] for x in lanes]
    down += [w[z.r - 8 : z.r, x] for x in lanes]
    odd = place[2]
    for v, (u, d) in enumerate(zip(up, down)):
        cor_a[v] = jnp.where(odd == 0, d, u)
        cor_b[v] = jnp.where(odd == 0, u, d)
    sums[...] = jnp.zeros_like(sums)
    first_q(z, ne, [(M, M + z.r - 1)], qx, qy, acc, sums)


def first_q(z, ne, runs, qx, qy, acc, sums):
    across, along = masks(z)
    acc[...] = jnp.zeros_like(acc)

    def band_tile(t, _):
        for lo, hi in runs:
            here = ne[NE0 + lo, t]
            for e in range(lo, hi):
                below_row = ne[NE0 + e + 1, t]
                gx = across(e, below_row - here)
                gy = along(pltpu.roll(here, z.ec - 1, axis=1) - here)
                qx[QX0 + e, t] = gx
                qy[QY0 + e, t] = gy
                acc[e] = acc[e] + (gx * gx + gy * gy)
                here = below_row
        return 0

    lax.fori_loop(0, z.bt, band_tile, 0)
    for lo, hi in runs:
        for e in range(lo, hi):
            sums[e : e + 1, :] = jnp.sum(acc[e], axis=0, keepdims=True)


def masks(z):
    row, half = lax.axis_index("row"), here()[1]
    rows = {
        M - 1: jnp.where(row > 0, 1.0, 0.0),
        M + z.r - 1: jnp.where(row < lax.axis_size("row") - 1, 1.0, 0.0),
    }
    cut = z.c - LANES
    lane = lane_iota((8, z.ec - cut)) + cut
    col = lax.axis_index("col") * (2 * z.c) + half * z.c + jnp.where(lane < z.c + LANES // 2, lane, lane - z.ec)
    tail = jnp.where((col >= 0) & (col < lax.axis_size("col") * (2 * z.c) - 1), 1.0, 0.0)

    def across(e, d):
        return d * rows[e] if e in rows else d

    def along(d):
        return jnp.concatenate([d[:, 0:cut], d[:, cut : z.ec] * tail], axis=1)

    return across, along


def message_rows(z, k):
    lo, hi = k, z.er - 1 - k
    return lo, hi - lo + (hi - lo) % 2


def message_shape(z, k):
    return (message_rows(z, k)[1] * (z.c // LANES) + 8, LANES)


def write_message(z, k, acc, sums, msg):
    lo, hi = k, z.er - 1 - k
    sums[...] = jnp.zeros_like(sums)
    for e in range(lo, hi):
        sums[e : e + 1, :] = jnp.sum(acc[e], axis=0, keepdims=True)
    pack_message(z, k, sums, msg)


def pack_message(z, k, sums, msg):
    first, n = message_rows(z, k)
    for t in range(z.c // LANES):
        msg[t * n : (t + 1) * n, :] = sums[first : first + n, t * LANES : (t + 1) * LANES]
    halo = [sums[8 * g : 8 * g + 8, z.c : z.ec] for g in range(z.er // 8)]
    msg[n * (z.c // LANES) :, :] = pack_lanes(halo, LANES - M, 2 * M)[0]


def read_scale(z, k, msg_a, msg_b, wx, sums, scale):
    lo, hi = k, z.er - 1 - k
    first, n = message_rows(z, k)
    lane = lane_iota((8, LANES))
    sums[...] = jnp.zeros_like(sums)
    for t in range(z.c // LANES):
        part = slice(t * n, (t + 1) * n)
        sums[first : first + n, t * LANES : (t + 1) * LANES] = msg_a[part, :] + msg_b[part, :]
    packed = msg_a[n * (z.c // LANES) :, :] + msg_b[n * (z.c // LANES) :, :]
    for g in range(z.er // 8):
        got = pltpu.roll(packed, (LANES - M - g * 2 * M) % LANES, axis=1)
        sums[8 * g : 8 * g + 8, z.c : z.ec] = jnp.where((lane < M) | (lane >= LANES - M), got, 0.0)
    w = wx[...]
    sums[...] = w / jnp.maximum(w, jnp.sqrt(1.0 + (SIGMA * SIGMA) * sums[...]))
    for e in range(lo, hi):
        scale[e] = jnp.broadcast_to(sums[e : e + 1, :], (8, z.ec))


def frame_rows(z, place, ne_in, qx_in, qy_in, wx_in, sums_in, a_keep, a_send, b_keep, b_send, cor_a, cor_b, ne, qx, qy, wx, msg, acc, sums):
    core, odd = place[0], place[2]
    lane = lane_iota((8, LANES))
    sub = lax.broadcasted_iota(jnp.int32, (8, z.c), 0)
    per = LANES // (2 * M)
    q4 = z.rest

    for keep, send, first in ((a_keep, a_send, (1 - odd) * (M + z.r)), (b_keep, b_send, odd * (M + z.r))):
        for i in range(M):
            e = NE0 + first + i
            for bt in range(z.ft):
                ne[e, core * z.ft + bt, :, 0 : z.c] = keep[z.ft * i + bt]
                ne[e, (1 - core) * z.ft + bt, :, 0 : z.c] = send[z.ft * i + bt]
            k, s = keep[z.ft * M + i // 2], send[z.ft * M + i // 2]
            k0, s0 = jnp.where(core == 0, k, s), jnp.where(core == 0, s, k)
            if i % 2 == 0:
                s0 = pltpu.roll(s0, q4, axis=0)
            else:
                k0 = pltpu.roll(k0, q4, axis=0)
            ne[e, 2 * z.ft, :, 0 : z.c] = jnp.where(sub < q4, k0, s0)

    n_cor = cor_a.shape[0] - z.lt
    below = [jnp.where(odd == 0, cor_a[v], cor_b[v]) for v in range(n_cor + z.lt)]
    above = [jnp.where(odd == 0, cor_b[v], cor_a[v]) for v in range(n_cor + z.lt)]

    def corner(got, k):
        v, p = divmod(k, per)
        moved = pltpu.roll(got[v], (LANES - M - p * 2 * M) % LANES, axis=1)
        return jnp.where((lane < M) | (lane >= LANES - M), moved, 0.0)

    for r in range(M):
        for t in range(z.bt):
            ne[NE0 + M + z.r + r, t, :, z.c : z.ec] = corner(below, r * z.bt + t)
            ne[NE0 + r, t, :, z.c : z.ec] = corner(above, r * z.bt + t)
    wx[...] = wx_in[...]
    for t in range(z.lt):
        lanes = slice(t * LANES, (t + 1) * LANES)
        wx[M + z.r : z.er, lanes] = below[n_cor + t][0:M]
        wx[0:M, lanes] = above[n_cor + t][8 - M : 8]
    wx[M + z.r : z.er, z.c : z.ec] = corner(below, M * z.bt)[0:M]
    wx[0:M, z.c : z.ec] = corner(above, M * z.bt)[8 - M : 8]
    sums[...] = sums_in[...]
    first_q(z, ne, [(0, M), (M + z.r - 1, z.er - 1)], qx, qy, acc, sums)
    pack_message(z, 0, sums, msg)


CARRY = 1.0 / (1.0 + TAU)
GAIN = TAU / (1.0 + TAU)


def rest_of_update(z, k, ne, u, base):
    def band_tile(t, _):
        for e in range(k + 1, z.er - 1 - k):
            base[NE0 + e, t] = CARRY * u[U0 + e, t] + GAIN * ne[NE0 + e, t]
        return 0

    lax.fori_loop(0, z.bt, band_tile, 0)


def step(z, k, base, wx, u_in, qx_in, qy_in, msg_a, msg_b, u, qx, qy, msg, sums, scale, acc, ubs, pxs, pys):
    lo, hi = k, z.er - 1 - k
    read_scale(z, k, msg_a, msg_b, wx, sums, scale)
    acc[...] = jnp.zeros_like(acc)
    across, along = masks(z)

    def band_tile(t, _):
        px0 = scale[lo] * qx_in[QX0 + lo, t]
        for e in range(lo + 1, hi):
            sc = scale[e]
            px = sc * qx_in[QX0 + e, t]
            py = sc * qy_in[QY0 + e, t]
            div = ((px - px0) + py) - pltpu.roll(py, 1, axis=1)
            old = u_in[(NE0 if k == 0 else U0) + e, t]
            new = (old if k == 0 else base[NE0 + e, t]) + (GAIN * SIGMA) * div
            u[U0 + e, t] = new
            ubs[e] = (new - old) + new
            pxs[e], pys[e] = px, py
            px0 = px
        ub0 = ubs[lo + 1]
        for e in range(lo + 1, hi - 1):
            ub = ubs[e + 1]
            nx = pxs[e] + across(e, ub - ub0)
            ny = pys[e] + along(pltpu.roll(ub0, z.ec - 1, axis=1) - ub0)
            qx[QX0 + e, t] = nx
            qy[QY0 + e, t] = ny
            acc[e] = acc[e] + (nx * nx + ny * ny)
            ub0 = ub
        return 0

    lax.fori_loop(0, z.bt, band_tile, 0)
    write_message(z, k + 1, acc, sums, msg)


def last_step(z, k, own, place, base, wx, qx_in, qy_in, msg_a, msg_b, *refs):
    part = refs[0]
    sums, scale, u = refs[-3:]
    lo, hi = k, z.er - 1 - k
    core = place[0]
    slot = (core if own else 1 - core) * z.ft
    q4 = z.rest
    read_scale(z, k, msg_a, msg_b, wx, sums, scale)

    def band_tile(i, _):
        t = jnp.where(i == z.ft, 2 * z.ft, slot + i)
        px0 = scale[lo] * qx_in[QX0 + lo, t]
        for e in range(lo + 1, hi):
            sc = scale[e]
            px = sc * qx_in[QX0 + e, t]
            py = sc * qy_in[QY0 + e, t]
            div = ((px - px0) + py) - pltpu.roll(py, 1, axis=1)
            new = base[NE0 + e, t] + (GAIN * SIGMA) * div
            u[e - M, i] = new[:, 0 : z.c]
            px0 = px
        return 0

    lax.fori_loop(0, z.ft + 1, band_tile, 0)
    low = (core == 0) if own else (core == 1)
    for r in range(z.r):
        g, q = divmod(r, 8)
        for t in range(z.lt):
            lanes = slice(t * LANES, (t + 1) * LANES)
            run = flat_rows(part, g, t)
            for bt in range(z.ft):
                run[pl.ds(64 * bt + q, 8, stride=8), :] = u[r, bt, :, lanes]
            a, b = u[r, z.ft, 0:q4, lanes], u[r, z.ft, q4:8, lanes]
            run[pl.ds(8 * z.full + q, q4, stride=8), :] = jnp.where(low, a, b)


def write_half(z, own, place, block, *refs):
    out, sem = refs[-2:]
    copies = half_copies(z, place[1] if own else 1 - place[1], out, block, sem, out=True)
    for c in copies:
        c.start()
    for c in copies:
        c.wait()


def local(noisy, weight_map):
    z = Sizes(*noisy.shape)
    n_row, n_col, n_band = (lax.axis_size(a) for a in ("row", "col", "band"))
    chips = n_band // 2

    def at(chip, h):
        return 2 * chip + (h ^ (chip % 2))

    swap = [(i, i ^ 1) for i in range(n_band)]
    pair_a = [(at(c, h), at(c ^ 1, h)) for c in range(chips) for h in range(2)]
    pair_b = [(at(c, h), at((c - 1 + 2 * (c % 2)) % chips, h)) for c in range(chips) for h in range(2)]
    rows_a = [(i, i ^ 1) for i in range(n_row)]
    rows_b = [(i, min(max(i - 1 + 2 * (i % 2), 0), n_row - 1)) for i in range(n_row)]
    across_a = [(i * n_band + b, j * n_band + (b ^ 1)) for i, j in rows_a for b in range(n_band)]
    across_b = [(i * n_band + b, j * n_band + (b ^ 1)) for i, j in rows_b for b in range(n_band)]
    spot = [[(j // 2) * n_band + at(c, j % 2) for j in range(2 * n_col)] for c in range(chips)]
    to_right = [(line[j], line[(j + 1) % len(line)]) for line in spot for j in range(len(line))]
    to_left = [(b, a) for a, b in to_right]


    units = z.r * z.bt + z.r // 8
    n_edge = -(-units // (LANES // M))
    n_corner = -(-(M * z.bt + 1) // (LANES // (2 * M)))
    state = (z.er + 4, z.bt, 8, z.ec)
    flat = (z.er, z.ec)
    side = (n_edge, 8, LANES)
    bulk = (z.ft * M + M * z.rest // 8, 8, z.c)
    corner = (n_corner + z.lt, 8, LANES)
    cost = z.er * z.nb * z.ec
    sem = pltpu.SemaphoreType.DMA((z.rg * z.lt,))

    block = (z.lt, z.b, 8, LANES)
    sem_g = pltpu.SemaphoreType.DMA((z.lt,))
    cube, weights = (pltpu.with_memory_space_constraint(x, pltpu.HBM) for x in (noisy, weight_map))
    parts, far = [], []
    for name, same, cross in (("a", rows_a, across_a), ("b", rows_b, across_b)):
        b = name == "b"
        keep, send, msg_keep, msg_send, *w = call(
            lambda *a, b=b: split(z, b, here(), *a), [block, block, bulk, bulk] + [(z.r, z.c)] * b,
            [cube] + [weights] * b, scratch=[sem_g, sem_g] + [pltpu.SemaphoreType.DMA] * b,
            hbm_in=(0, 1), flops=cost,
        )
        far.append(lax.ppermute(msg_keep, "row", same))
        far.append(lax.ppermute(msg_send, ("row", "band"), cross))
        parts += [keep, lax.ppermute(send, "band", swap)]
    (w,) = w
    ne, col_l, col_r = call(
        lambda *a: assemble(z, here(), *a), [state, side, side], [*parts, w], flops=cost
    )
    from_r = lax.ppermute(col_l, ("col", "band"), to_left)
    from_l = lax.ppermute(col_r, ("col", "band"), to_right)
    acc = pltpu.VMEM((z.er, 8, z.ec), F32)
    one = pltpu.VMEM(flat, F32)
    ne, wx, qx, qy, sums, cor_a, cor_b = call(
        lambda *a: frame_cols(z, here(), *a), [state, flat, state, state, flat, corner, corner],
        [ne, w, from_r, from_l], aliases={0: 0}, scratch=[acc], flops=5 * cost,
    )
    cor_a = lax.ppermute(cor_a, "row", rows_a)
    cor_b = lax.ppermute(cor_b, "row", rows_b)
    ne, qx, qy, wx, msg = call(
        lambda *a: frame_rows(z, here(), *a), [state, state, state, flat, message_shape(z, 0)],
        [ne, qx, qy, wx, sums, *far, cor_a, cor_b],
        aliases={0: 0, 1: 1, 2: 2}, scratch=[acc, one], flops=5 * cost,
    )
    u = base = ne
    for k in range(ITERS):
        pairs = (pair_a, pair_b) if k % 2 == 0 else (pair_b, pair_a)
        msg = msg + lax.ppermute(msg, "band", pairs[0])
        other = lax.ppermute(msg, "band", pairs[1])
        if k > 0:
            (base,) = call(lambda *a, k=k: rest_of_update(z, k, *a), [state], [ne, u], flops=cost)
        if k < ITERS - 1:
            u, qx, qy, msg = call(
                lambda *a, k=k: step(z, k, *a), [state, state, state, message_shape(z, k + 1)],
                [base, wx, u, qx, qy, msg, other], scratch=[one, acc, acc, acc, acc, acc], flops=20 * cost,
            )
    last = [base, wx, qx, qy, msg, other]
    room = [one, acc, pltpu.VMEM((z.r, z.ft + 1, 8, z.c), F32)]
    (send,) = call(lambda *a: last_step(z, ITERS - 1, False, here(), *a), [z.block], last, scratch=room, flops=5 * cost)
    recv = lax.ppermute(send, "band", swap)
    (keep,) = call(lambda *a: last_step(z, ITERS - 1, True, here(), *a), [z.block], last, scratch=room, flops=5 * cost)
    (out,) = call(
        lambda *a: write_half(z, True, here(), *a), [noisy.shape], [keep], scratch=[sem], hbm_out=(0,), flops=cost
    )
    (out,) = call(
        lambda *a: write_half(z, False, here(), *a), [noisy.shape], [recv, out],
        aliases={1: 0}, scratch=[sem], hbm_in=(1,), hbm_out=(0,), flops=cost,
    )
    return out


def solution(mesh):
    placed = (P("band", "row", "col"), P("row", "col"))
    return jax.shard_map(local, mesh=mesh, in_specs=placed, out_specs=P("band", "row", "col"), check_vma=False)
```
